128 devices in a mesh: tp: 4 (over x), cp: 32 (over z, y, core).
Axes of the slice: x: 4, y: 4, z: 4, core: 2. Of those that a mesh axis runs over, the one named last changes fastest.
Arguments:
- x_in: bfloat16 [8192, 4096], P('cp')
- positions: int32 [8192], P('cp')
- attn_gain: bfloat16 [2, 4096], replicated
- mlp_gain: bfloat16 [2, 4096], replicated
- w_query: bfloat16 [2, 4096, 4096], P(None, None, 'tp')
- b_query: bfloat16 [2, 4096], P(None, 'tp')
- w_key: bfloat16 [2, 4096, 4096], P(None, None, 'tp')
- b_key: bfloat16 [2, 4096], P(None, 'tp')
- w_value: bfloat16 [2, 4096, 4096], P(None, None, 'tp')
- b_value: bfloat16 [2, 4096], P(None, 'tp')
- w_out: bfloat16 [2, 4096, 4096], P(None, 'tp')
- w_gate: bfloat16 [2, 4096, 11008], P(None, None, 'tp')
- w_up: bfloat16 [2, 4096, 11008], P(None, None, 'tp')
- w_down: bfloat16 [2, 11008, 4096], P(None, 'tp')
Outputs:
- output 1: bfloat16 [8192, 4096], P('cp')
- output 2: bfloat16 [8192, 32, 128], P('cp', 'tp')
- output 3: bfloat16 [8192, 32, 128], P('cp', 'tp')
- output 4: bfloat16 [8192, 32, 128], P('cp', 'tp')
- output 5: bfloat16 [8192, 32, 128], P('cp', 'tp')
All inputs are finite; a program needn't handle non-finite values.
Results may differ from the reference program's by a relative error of at most 0.02.
Values are sent between devices in bfloat16 or wider.
A program may use at most 1 GiB of HBM per device.

```python
import jax
import jax.numpy as jnp
from jax import lax

TOKENS = 8192
HIDDEN = 4096
Q_HEADS = 32
KV_HEADS = 32
HEAD_DIM = 128
FFN_DIM = 11008
WINDOW = 4096


def setup_inputs(seed: int = 0) -> dict:
    key_list = jax.random.split(jax.random.key(seed), 14)
    q_width = Q_HEADS * HEAD_DIM
    kv_width = KV_HEADS * HEAD_DIM

    def normal_draw(key_idx, arr_shape, factor):
        return (jax.random.normal(key_list[key_idx], arr_shape, jnp.float32) * factor).astype(jnp.bfloat16)

    def gain_draw(key_idx):
        return jax.random.uniform(key_list[key_idx], (2, HIDDEN), jnp.float32, 0.5, 1.5).astype(jnp.bfloat16)

    pos_start = jax.random.randint(key_list[1], (), 0, 8192, jnp.int32)
    return {
        'x_in': normal_draw(0, (TOKENS, HIDDEN), 1.0),
        'positions': pos_start + jnp.arange(TOKENS, dtype=jnp.int32),
        'attn_gain': gain_draw(2),
        'mlp_gain': gain_draw(3),
        'w_query': normal_draw(4, (2, HIDDEN, q_width), 2.0 * HIDDEN ** -0.5),
        'b_query': normal_draw(5, (2, q_width), 0.5),
        'w_key': normal_draw(6, (2, HIDDEN, kv_width), 2.0 * HIDDEN ** -0.5),
        'b_key': normal_draw(7, (2, kv_width), 0.5),
        'w_value': normal_draw(8, (2, HIDDEN, kv_width), HIDDEN ** -0.5),
        'b_value': normal_draw(9, (2, kv_width), 0.5),
        'w_out': normal_draw(10, (2, q_width, HIDDEN), 2.0 * q_width ** -0.5),
        'w_gate': normal_draw(11, (2, HIDDEN, FFN_DIM), HIDDEN ** -0.5),
        'w_up': normal_draw(12, (2, HIDDEN, FFN_DIM), HIDDEN ** -0.5),
        'w_down': normal_draw(13, (2, FFN_DIM, HIDDEN), FFN_DIM ** -0.5),
    }


def rms_norm(hidden, gain):
    hidden_f = hidden.astype(jnp.float32)
    variance = jnp.mean(hidden_f * hidden_f, axis=-1, keepdims=True)
    return (hidden_f * lax.rsqrt(variance + 1e-6) * gain.astype(jnp.float32)).astype(jnp.bfloat16)


def rope_tables(positions):
    inv_freq = 1.0 / (1000000.0 ** (jnp.arange(0, HEAD_DIM, 2, dtype=jnp.float32) / HEAD_DIM))
    angles = positions.astype(jnp.float32)[:, None] * inv_freq[None, :]
    return jnp.cos(angles)[:, None, :], jnp.sin(angles)[:, None, :]


def apply_rope(proj_f, cos_tab, sin_tab):
    half_dim = proj_f.shape[-1] // 2
    first_half = proj_f[..., :half_dim]
    second_half = proj_f[..., half_dim:]
    return jnp.concatenate([first_half * cos_tab - second_half * sin_tab, second_half * cos_tab + first_half * sin_tab], axis=-1)


def project(normed, weight, bias_vec):
    return jnp.dot(normed, weight, preferred_element_type=jnp.float32) + bias_vec.astype(jnp.float32)


def attention(queries, key_cache, value_cache, window):
    group_size = Q_HEADS // KV_HEADS
    block_len = 128
    block_count = TOKENS // block_len
    q_blocks = queries.reshape(block_count, block_len, KV_HEADS, group_size, HEAD_DIM).astype(jnp.float32)
    keys_f = key_cache.astype(jnp.float32)
    values_f = value_cache.astype(jnp.float32)
    key_pos = jnp.arange(TOKENS)
    score_scale = HEAD_DIM ** -0.5

    def one_block(block_in):
        block_idx, q_blk = block_in
        query_pos = block_idx * block_len + jnp.arange(block_len)
        scores = jnp.einsum('qkgd,skd->qkgs', q_blk, keys_f) * score_scale
        allowed = (key_pos[None, :] <= query_pos[:, None]) & (key_pos[None, :] > query_pos[:, None] - window)
        scores = jnp.where(allowed[:, None, None, :], scores, -jnp.inf)
        probs = jax.nn.softmax(scores, axis=-1).astype(jnp.bfloat16).astype(jnp.float32)
        return jnp.einsum('qkgs,skd->qkgd', probs, values_f).astype(jnp.bfloat16)

    attn_out = lax.map(one_block, (jnp.arange(block_count), q_blocks))
    return attn_out.reshape(TOKENS, Q_HEADS * HEAD_DIM)


def reference(x_in, positions, attn_gain, mlp_gain, w_query, b_query, w_key, b_key, w_value, b_value, w_out, w_gate, w_up, w_down):
    cos_tab, sin_tab = rope_tables(positions)
    hidden = x_in
    caches = []
    for layer_idx, window in ((0, TOKENS), (1, WINDOW)):
        normed = rms_norm(hidden, attn_gain[layer_idx])
        queries = apply_rope(project(normed, w_query[layer_idx], b_query[layer_idx]).reshape(TOKENS, Q_HEADS, HEAD_DIM), cos_tab, sin_tab).astype(jnp.bfloat16)
        key_cache = apply_rope(project(normed, w_key[layer_idx], b_key[layer_idx]).reshape(TOKENS, KV_HEADS, HEAD_DIM), cos_tab, sin_tab).astype(jnp.bfloat16)
        value_cache = project(normed, w_value[layer_idx], b_value[layer_idx]).astype(jnp.bfloat16).reshape(TOKENS, KV_HEADS, HEAD_DIM)
        attn_out = attention(queries, key_cache, value_cache, window)
        hidden = (hidden.astype(jnp.float32) + jnp.dot(attn_out, w_out[layer_idx], preferred_element_type=jnp.float32)).astype(jnp.bfloat16)
        normed = rms_norm(hidden, mlp_gain[layer_idx])
        gate_proj = jnp.dot(normed, w_gate[layer_idx], preferred_element_type=jnp.float32)
        up_proj = jnp.dot(normed, w_up[layer_idx], preferred_element_type=jnp.float32)
        activated = (jax.nn.silu(gate_proj) * up_proj).astype(jnp.bfloat16)
        hidden = (hidden.astype(jnp.float32) + jnp.dot(activated, w_down[layer_idx], preferred_element_type=jnp.float32)).astype(jnp.bfloat16)
        caches.append(key_cache)
        caches.append(value_cache)
    return (hidden, caches[0], caches[1], caches[2], caches[3])
```

```python
import functools

import jax
import jax.numpy as jnp
from jax import lax
from jax.experimental import pallas as pl
from jax.experimental.pallas import tpu as pltpu
from jax.sharding import PartitionSpec as P

HEAD_DIM = 128
WINDOW = 4096
MESH = pl.DeviceIdType.MESH
NEG = -0.7 * float(jnp.finfo(jnp.float32).max)
LOG2E = 1.4426950408889634
MIB = 1024 * 1024


def rms_norm(hidden, gain):
    hidden_f = hidden.astype(jnp.float32)
    variance = jnp.mean(hidden_f * hidden_f, axis=-1, keepdims=True)
    return (hidden_f * lax.rsqrt(variance + 1e-6) * gain.astype(jnp.float32)).astype(jnp.bfloat16)


def rope_tables(positions):
    inv_freq = 1.0 / (1000000.0 ** (jnp.arange(0, HEAD_DIM, 2, dtype=jnp.float32) / HEAD_DIM))
    angles = positions.astype(jnp.float32)[:, None] * inv_freq[None, :]
    cos, sin = jnp.cos(angles), jnp.sin(angles)
    return jnp.concatenate([cos, cos], axis=-1), jnp.concatenate([-sin, sin], axis=-1)


def qkv_kernel(x_ref, gain_ref, cos_ref, sin_ref, wq_ref, bq_ref, wk_ref, bk_ref, wv_ref, bv_ref, q_ref, kv_ref, normed):
    @pl.when(pl.program_id(0) == 0)
    def _():
        normed[...] = rms_norm(x_ref[...], gain_ref[...])

    hidden = normed[...]
    cos_tab, sin_tab = cos_ref[...], sin_ref[...]

    def project(w_ref, b_ref):
        return jnp.dot(hidden, w_ref[...], preferred_element_type=jnp.float32) + b_ref[...].astype(jnp.float32)

    def rope(proj):
        heads = []
        for start in range(0, proj.shape[1], HEAD_DIM):
            head = proj[:, start:start + HEAD_DIM]
            heads.append(head * cos_tab + pltpu.roll(head, HEAD_DIM // 2, 1) * sin_tab)
        return jnp.concatenate(heads, axis=1).astype(jnp.bfloat16)

    q_ref[...] = rope(project(wq_ref, bq_ref))
    kv_ref[0] = rope(project(wk_ref, bk_ref))
    kv_ref[1] = project(wv_ref, bv_ref).astype(jnp.bfloat16)


def qkv_project(layer, hidden, gains, cos_tab, sin_tab, w_query, b_query, w_key, b_key, w_value, b_value, tile=256):
    rows, width = hidden.shape
    cols = w_query.shape[2]
    whole = lambda shape: pl.BlockSpec(shape, lambda n: (0,) * len(shape))
    weight = pl.BlockSpec((None, width, tile), lambda n: (layer, 0, n))
    bias = pl.BlockSpec((1, tile), lambda n: (0, n))
    return pl.pallas_call(
        qkv_kernel,
        grid=(cols // tile,),
        out_shape=(jax.ShapeDtypeStruct((rows, cols), jnp.bfloat16), jax.ShapeDtypeStruct((2, rows, cols), jnp.bfloat16)),
        in_specs=[whole((rows, width)), whole((1, width)), whole(cos_tab.shape), whole(sin_tab.shape), weight, bias, weight, bias, weight, bias],
        out_specs=(pl.BlockSpec((rows, tile), lambda n: (0, n)), pl.BlockSpec((2, rows, tile), lambda n: (0, 0, n))),
        scratch_shapes=[pltpu.VMEM((rows, width), jnp.bfloat16)],
        compiler_params=pltpu.CompilerParams(vmem_limit_bytes=40 * MIB),
        cost_estimate=pl.CostEstimate(flops=6 * rows * width * cols, bytes_accessed=6 * width * cols, transcendentals=0),
        name='qkv',
    )(hidden, gains[layer:layer + 1], cos_tab, sin_tab, w_query, b_query[layer:layer + 1], w_key, b_key[layer:layer + 1], w_value, b_value[layer:layer + 1])


def attention_kernel(cp_size, window, q_ref, kv_ref, out_ref, kvbuf, qbuf, obuf, acc, m_buf, l_buf,
                     kv_send, kv_recv, fwd_send, q_send, q_recv, o_send, o_recv):
    rows = q_ref.shape[0]
    n_heads = q_ref.shape[1] // HEAD_DIM
    chips = cp_size // 2
    groups = cp_size // n_heads
    slots = cp_size // groups
    me = lax.axis_index('cp')
    chip, core = me // 2, lax.rem(me, 2)
    head, group = me // groups, lax.rem(me, groups)
    sibling = me + 1 - 2 * core
    scale = HEAD_DIM ** -0.5 * LOG2E

    def lanes(h):
        return pl.ds(pl.multiple_of(h * HEAD_DIM, HEAD_DIM), HEAD_DIM)

    def block_of(slot):
        odd = lax.rem(slot, 2)
        return 2 * groups * (slot // 2) + group + odd * (2 * groups - 1 - 2 * group)

    barrier = pltpu.get_barrier_semaphore()

    @pl.loop(1, cp_size)
    def _(step):
        pl.semaphore_signal(barrier, inc=1, device_id={'cp': lax.rem(me + step, cp_size)}, device_id_type=MESH)

    own_kv = pltpu.make_async_copy(kv_ref.at[:, :, lanes(head)], kvbuf.at[me], kv_recv.at[me])
    own_kv.start()
    pl.semaphore_wait(barrier, cp_size - 1)

    place = lax.rem(me, 2 * groups)
    upper = place // groups
    my_group = place + upper * (2 * groups - 1 - 2 * place)
    my_slot = 2 * (me // (2 * groups)) + upper

    def q_copy(h):
        return pltpu.make_async_remote_copy(q_ref.at[:, lanes(h)], qbuf.at[my_slot], q_send.at[h], q_recv.at[my_slot],
                                            device_id={'cp': groups * h + my_group}, device_id_type=MESH)

    def kv_copy(dst):
        return pltpu.make_async_remote_copy(kv_ref.at[:, :, lanes((2 * dst) // groups)], kvbuf.at[me], kv_send.at[dst], kv_recv.at[me],
                                            device_id={'cp': 2 * dst + core}, device_id_type=MESH)

    def fwd_copy(src):
        blk = 2 * src + core
        return pltpu.make_async_remote_copy(kvbuf.at[blk], kvbuf.at[blk], fwd_send.at[src], kv_recv.at[blk],
                                            device_id={'cp': sibling}, device_id_type=MESH)

    def kv_wait(blk):
        pltpu.make_async_copy(kvbuf.at[blk], kvbuf.at[blk], kv_recv.at[blk]).wait()

    @pl.loop(0, n_heads)
    def _(h):
        @pl.when(groups * h + my_group != me)
        def _():
            q_copy(h).start()

        @pl.when(groups * h + my_group == me)
        def _():
            pltpu.make_async_copy(q_ref.at[:, lanes(h)], qbuf.at[my_slot], q_recv.at[my_slot]).start()

    @pl.loop(1, chips)
    def _(step):
        kv_copy(lax.rem(chip + step, chips)).start()

    kv_wait(me)
    fwd_copy(chip).start()

    acc[...] = jnp.zeros_like(acc)
    l_buf[...] = jnp.zeros_like(l_buf)
    m_buf[...] = jnp.full_like(m_buf, NEG)

    @pl.loop(0, slots)
    def _(slot):
        pltpu.make_async_copy(qbuf.at[slot], qbuf.at[slot], q_recv.at[slot]).wait()

    def attend(slot, src, masked):
        keys = kvbuf[pl.ds(2 * src, 2), 0].reshape(2 * rows, HEAD_DIM)
        values = kvbuf[pl.ds(2 * src, 2), 1].reshape(2 * rows, HEAD_DIM)
        scores = lax.dot_general(qbuf[slot], keys, (((1,), (1,)), ((), ())), preferred_element_type=jnp.float32) * scale
        if masked:
            q_pos = block_of(slot) * rows + lax.broadcasted_iota(jnp.int32, scores.shape, 0)
            k_pos = src * 2 * rows + lax.broadcasted_iota(jnp.int32, scores.shape, 1)
            scores = jnp.where((k_pos <= q_pos) & (k_pos > q_pos - window), scores, NEG)
        parts = [scores[:, i:i + HEAD_DIM] for i in range(0, scores.shape[1], HEAD_DIM)] if scores.shape[1] % HEAD_DIM == 0 else [scores]
        m_prev = m_buf[slot]
        m_lane = functools.reduce(jnp.maximum, parts)
        m_new = jnp.maximum(m_prev, jnp.max(m_lane, axis=1, keepdims=True))
        alpha = jnp.exp2(m_prev - m_new)
        probs = [jnp.exp2(part - m_new[:, :part.shape[1]]) for part in parts]
        l_new = functools.reduce(jnp.add, probs)
        if l_new.shape[1] != HEAD_DIM:
            l_new = jnp.concatenate([l_new, jnp.zeros((rows, HEAD_DIM - l_new.shape[1]), jnp.float32)], axis=1)
        l_buf[slot] = alpha * l_buf[slot] + l_new
        m_buf[slot] = m_new
        probs_bf = jnp.concatenate([part.astype(jnp.bfloat16) for part in probs], axis=1)
        acc[slot] = alpha * acc[slot] + jnp.dot(probs_bf, values, preferred_element_type=jnp.float32)

    win_blocks = window // rows

    @pl.loop(1, chips + 1)
    def _(step):
        @pl.when(step < chips)
        def _():
            src = lax.rem(chip - step + chips, chips)
            kv_wait(2 * src + core)
            fwd_copy(src).start()

        src = lax.rem(chip - step + 1 + chips, chips)
        kv_wait(2 * src + 1 - core)

        @pl.loop(0, slots)
        def _(slot):
            blk = block_of(slot)
            diagonal = src == blk // 2
            edge = 2 * src <= blk - win_blocks
            inside = (2 * src <= blk) & (2 * src + 1 >= blk - win_blocks)

            @pl.when(inside & jnp.logical_not(diagonal | edge))
            def _():
                attend(slot, src, False)

            @pl.when(inside & (diagonal | edge))
            def _():
                attend(slot, src, True)

    @pl.loop(0, slots)
    def _(slot):
        total = jnp.sum(l_buf[slot], axis=1, keepdims=True)
        obuf[slot] = (acc[slot] / total).astype(jnp.bfloat16)

    def o_copy(slot):
        return pltpu.make_async_remote_copy(obuf.at[slot], out_ref.at[:, lanes(head)], o_send.at[slot], o_recv.at[head],
                                            device_id={'cp': block_of(slot)}, device_id_type=MESH)

    @pl.loop(0, slots)
    def _(slot):
        @pl.when(block_of(slot) != me)
        def _():
            o_copy(slot).start()

        @pl.when(block_of(slot) == me)
        def _():
            pltpu.make_async_copy(obuf.at[slot], out_ref.at[:, lanes(head)], o_recv.at[head]).start()

    @pl.loop(0, n_heads)
    def _(h):
        pltpu.make_async_copy(out_ref.at[:, lanes(h)], out_ref.at[:, lanes(h)], o_recv.at[h]).wait()

        @pl.when(groups * h + my_group != me)
        def _():
            q_copy(h).wait_send()

    @pl.loop(0, slots)
    def _(slot):
        @pl.when(block_of(slot) != me)
        def _():
            o_copy(slot).wait_send()

    @pl.loop(0, chips)
    def _(dst):
        fwd_copy(dst).wait_send()

        @pl.when(dst != chip)
        def _():
            kv_copy(dst).wait_send()


def attention(cp_size, window, collective_id, queries, kv):
    rows, cols = queries.shape
    n_heads = cols // HEAD_DIM
    slots = n_heads
    dma = pltpu.SemaphoreType.DMA
    any_spec = pl.BlockSpec(memory_space=pl.ANY)
    return pl.pallas_call(
        functools.partial(attention_kernel, cp_size, window),
        out_shape=jax.ShapeDtypeStruct((rows, cols), jnp.bfloat16),
        in_specs=[any_spec, any_spec],
        out_specs=any_spec,
        scratch_shapes=[
            pltpu.VMEM((cp_size, 2, rows, HEAD_DIM), jnp.bfloat16),
            pltpu.VMEM((slots, rows, HEAD_DIM), jnp.bfloat16),
            pltpu.VMEM((slots, rows, HEAD_DIM), jnp.bfloat16),
            pltpu.VMEM((slots, rows, HEAD_DIM), jnp.float32),
            pltpu.VMEM((slots, rows, HEAD_DIM), jnp.float32),
            pltpu.VMEM((slots, rows, HEAD_DIM), jnp.float32),
            dma((cp_size // 2,)), dma((cp_size,)), dma((cp_size // 2,)),
            dma((n_heads,)), dma((slots,)), dma((slots,)), dma((n_heads,)),
        ],
        compiler_params=pltpu.CompilerParams(collective_id=collective_id, has_side_effects=True, vmem_limit_bytes=24 * MIB),
        cost_estimate=pl.CostEstimate(flops=4 * 132 * rows * rows * HEAD_DIM, bytes_accessed=8 * MIB, transcendentals=132 * rows * rows),
        name='attention',
    )(queries, kv)


def solution(mesh):
    cp_size = mesh.shape['cp']

    def local_step(x_in, positions, attn_gain, mlp_gain, w_query, b_query, w_key, b_key, w_value, b_value, w_out, w_gate, w_up, w_down):
        block_dev = x_in.shape[0]
        cos_tab, sin_tab = rope_tables(positions)
        hidden = x_in
        caches = []
        for layer_idx, window in ((0, block_dev * cp_size), (1, WINDOW)):
            queries, kv = qkv_project(layer_idx, hidden, attn_gain, cos_tab, sin_tab, w_query, b_query, w_key, b_key, w_value, b_value)
            attn_out = attention(cp_size, window, layer_idx, queries, kv)
            attn_part = jnp.dot(attn_out, w_out[layer_idx], preferred_element_type=jnp.float32).astype(jnp.bfloat16)
            hidden = (hidden.astype(jnp.float32) + lax.psum(attn_part, 'tp').astype(jnp.float32)).astype(jnp.bfloat16)
            normed = rms_norm(hidden, mlp_gain[layer_idx])
            gate_proj = jnp.dot(normed, w_gate[layer_idx], preferred_element_type=jnp.float32)
            up_proj = jnp.dot(normed, w_up[layer_idx], preferred_element_type=jnp.float32)
            activated = (jax.nn.silu(gate_proj) * up_proj).astype(jnp.bfloat16)
            down_part = jnp.dot(activated, w_down[layer_idx], preferred_element_type=jnp.float32).astype(jnp.bfloat16)
            hidden = (hidden.astype(jnp.float32) + lax.psum(down_part, 'tp').astype(jnp.float32)).astype(jnp.bfloat16)
            caches.append(kv[0].reshape(block_dev, -1, HEAD_DIM))
            caches.append(kv[1].reshape(block_dev, -1, HEAD_DIM))
        return hidden, caches[0], caches[1], caches[2], caches[3]

    weight_col = P(None, None, 'tp')
    bias_col = P(None, 'tp')
    weight_row = P(None, 'tp', None)
    replicated = P(None, None)
    cache_spec = P('cp', 'tp', None)
    in_specs = (P('cp', None), P('cp'), replicated, replicated, weight_col, bias_col, weight_col, bias_col, weight_col, bias_col, weight_row, weight_col, weight_col, weight_row)
    out_specs = (P('cp', None), cache_spec, cache_spec, cache_spec, cache_spec)
    return jax.shard_map(local_step, mesh=mesh, in_specs=in_specs, out_specs=out_specs, check_vma=False)
```

```python
import functools

import jax
import jax.numpy as jnp
from jax import lax
from jax.experimental import pallas as pl
from jax.experimental.pallas import tpu as pltpu
from jax.sharding import PartitionSpec as P

HEAD_DIM = 128
WINDOW = 4096
MESH = pl.DeviceIdType.MESH
NEG = -0.7 * float(jnp.finfo(jnp.float32).max)
LOG2E = 1.4426950408889634
MIB = 1024 * 1024


def rms_norm(hidden, gain):
    hidden_f = hidden.astype(jnp.float32)
    variance = jnp.mean(hidden_f * hidden_f, axis=-1, keepdims=True)
    return (hidden_f * lax.rsqrt(variance + 1e-6) * gain.astype(jnp.float32)).astype(jnp.bfloat16)


def rope_tables(positions):
    inv_freq = 1.0 / (1000000.0 ** (jnp.arange(0, HEAD_DIM, 2, dtype=jnp.float32) / HEAD_DIM))
    angles = positions.astype(jnp.float32)[:, None] * inv_freq[None, :]
    cos, sin = jnp.cos(angles), jnp.sin(angles)
    return jnp.concatenate([cos, cos], axis=-1), jnp.concatenate([-sin, sin], axis=-1)


def qkv_kernel(x_ref, gain_ref, cos_ref, sin_ref, wq_ref, bq_ref, wk_ref, bk_ref, wv_ref, bv_ref, q_ref, kv_ref, normed):
    @pl.when(pl.program_id(0) == 0)
    def _():
        normed[...] = rms_norm(x_ref[...], gain_ref[...])

    hidden = normed[...]
    cos_tab, sin_tab = cos_ref[...], sin_ref[...]

    def project(w_ref, b_ref):
        return jnp.dot(hidden, w_ref[...], preferred_element_type=jnp.float32) + b_ref[...].astype(jnp.float32)

    def rope(proj):
        heads = []
        for start in range(0, proj.shape[1], HEAD_DIM):
            head = proj[:, start:start + HEAD_DIM]
            heads.append(head * cos_tab + pltpu.roll(head, HEAD_DIM // 2, 1) * sin_tab)
        return jnp.concatenate(heads, axis=1).astype(jnp.bfloat16)

    q_ref[...] = rope(project(wq_ref, bq_ref))
    kv_ref[0] = rope(project(wk_ref, bk_ref))
    kv_ref[1] = project(wv_ref, bv_ref).astype(jnp.bfloat16)


def qkv_project(layer, hidden, gains, cos_tab, sin_tab, w_query, b_query, w_key, b_key, w_value, b_value, tile=256):
    rows, width = hidden.shape
    cols = w_query.shape[2]
    whole = lambda shape: pl.BlockSpec(shape, lambda n: (0,) * len(shape))
    weight = pl.BlockSpec((None, width, tile), lambda n: (layer, 0, n))
    bias = pl.BlockSpec((1, tile), lambda n: (0, n))
    return pl.pallas_call(
        qkv_kernel,
        grid=(cols // tile,),
        out_shape=(jax.ShapeDtypeStruct((rows, cols), jnp.bfloat16), jax.ShapeDtypeStruct((2, rows, cols), jnp.bfloat16)),
        in_specs=[whole((rows, width)), whole((1, width)), whole(cos_tab.shape), whole(sin_tab.shape), weight, bias, weight, bias, weight, bias],
        out_specs=(pl.BlockSpec((rows, tile), lambda n: (0, n)), pl.BlockSpec((2, rows, tile), lambda n: (0, 0, n))),
        scratch_shapes=[pltpu.VMEM((rows, width), jnp.bfloat16)],
        compiler_params=pltpu.CompilerParams(vmem_limit_bytes=40 * MIB),
        cost_estimate=pl.CostEstimate(flops=6 * rows * width * cols, bytes_accessed=6 * width * cols, transcendentals=0),
        name='qkv',
    )(hidden, gains[layer:layer + 1], cos_tab, sin_tab, w_query, b_query[layer:layer + 1], w_key, b_key[layer:layer + 1], w_value, b_value[layer:layer + 1])


def attention_kernel(cp_size, window, q_ref, kv_ref, out_ref, kvbuf, qbuf, obuf, acc, m_buf, l_buf,
                     kv_send, kv_recv, fwd_send, q_send, q_recv, o_send, o_recv):
    rows = q_ref.shape[0]
    n_heads = q_ref.shape[1] // HEAD_DIM
    chips = cp_size // 2
    groups = cp_size // n_heads
    slots = cp_size // groups
    me = lax.axis_index('cp')
    chip, core = me // 2, lax.rem(me, 2)
    head, group = me // groups, lax.rem(me, groups)
    sibling = me + 1 - 2 * core
    scale = HEAD_DIM ** -0.5 * LOG2E

    def lanes(h):
        return pl.ds(pl.multiple_of(h * HEAD_DIM, HEAD_DIM), HEAD_DIM)

    def block_of(slot):
        odd = lax.rem(slot, 2)
        return 2 * groups * (slot // 2) + group + odd * (2 * groups - 1 - 2 * group)

    barrier = pltpu.get_barrier_semaphore()

    @pl.loop(1, cp_size)
    def _(step):
        pl.semaphore_signal(barrier, inc=1, device_id={'cp': lax.rem(me + step, cp_size)}, device_id_type=MESH)

    own_kv = pltpu.make_async_copy(kv_ref.at[:, :, lanes(head)], kvbuf.at[me], kv_recv.at[me])
    own_kv.start()
    pl.semaphore_wait(barrier, cp_size - 1)

    place = lax.rem(me, 2 * groups)
    upper = place // groups
    my_group = place + upper * (2 * groups - 1 - 2 * place)
    my_slot = 2 * (me // (2 * groups)) + upper

    def q_copy(h):
        return pltpu.make_async_remote_copy(q_ref.at[:, lanes(h)], qbuf.at[my_slot], q_send.at[h], q_recv.at[my_slot],
                                            device_id={'cp': groups * h + my_group}, device_id_type=MESH)

    def kv_copy(dst):
        return pltpu.make_async_remote_copy(kv_ref.at[:, :, lanes((2 * dst) // groups)], kvbuf.at[me], kv_send.at[dst], kv_recv.at[me],
                                            device_id={'cp': 2 * dst + core}, device_id_type=MESH)

    def fwd_copy(src):
        blk = 2 * src + core
        return pltpu.make_async_remote_copy(kvbuf.at[blk], kvbuf.at[blk], fwd_send.at[src], kv_recv.at[blk],
                                            device_id={'cp': sibling}, device_id_type=MESH)

    def kv_wait(blk):
        pltpu.make_async_copy(kvbuf.at[blk], kvbuf.at[blk], kv_recv.at[blk]).wait()

    @pl.loop(0, n_heads)
    def _(h):
        @pl.when(groups * h + my_group != me)
        def _():
            q_copy(h).start()

        @pl.when(groups * h + my_group == me)
        def _():
            pltpu.make_async_copy(q_ref.at[:, lanes(h)], qbuf.at[my_slot], q_recv.at[my_slot]).start()

    @pl.loop(1, chips)
    def _(step):
        kv_copy(lax.rem(chip + step, chips)).start()

    kv_wait(me)
    fwd_copy(chip).start()

    acc[...] = jnp.zeros_like(acc)
    l_buf[...] = jnp.zeros_like(l_buf)
    m_buf[...] = jnp.full_like(m_buf, NEG)

    @pl.loop(0, slots)
    def _(slot):
        pltpu.make_async_copy(qbuf.at[slot], qbuf.at[slot], q_recv.at[slot]).wait()

    def attend(slot, src, masked):
        keys = kvbuf[pl.ds(2 * src, 2), 0].reshape(2 * rows, HEAD_DIM)
        values = kvbuf[pl.ds(2 * src, 2), 1].reshape(2 * rows, HEAD_DIM)
        scores = lax.dot_general(qbuf[slot], keys, (((1,), (1,)), ((), ())), preferred_element_type=jnp.float32) * scale
        if masked:
            q_pos = block_of(slot) * rows + lax.broadcasted_iota(jnp.int32, scores.shape, 0)
            k_pos = src * 2 * rows + lax.broadcasted_iota(jnp.int32, scores.shape, 1)
            scores = jnp.where((k_pos <= q_pos) & (k_pos > q_pos - window), scores, NEG)
        parts = [scores[:, i:i + HEAD_DIM] for i in range(0, scores.shape[1], HEAD_DIM)] if scores.shape[1] % HEAD_DIM == 0 else [scores]
        m_prev = m_buf[slot]
        m_lane = functools.reduce(jnp.maximum, parts)
        m_new = jnp.maximum(m_prev, jnp.max(m_lane, axis=1, keepdims=True))
        alpha = jnp.exp2(m_prev - m_new)
        probs = [jnp.exp2(part - m_new[:, :part.shape[1]]) for part in parts]
        l_new = functools.reduce(jnp.add, probs)
        if l_new.shape[1] != HEAD_DIM:
            l_new = jnp.concatenate([l_new, jnp.zeros((rows, HEAD_DIM - l_new.shape[1]), jnp.float32)], axis=1)
        l_buf[slot] = alpha * l_buf[slot] + l_new
        m_buf[slot] = m_new
        probs_bf = jnp.concatenate([part.astype(jnp.bfloat16) for part in probs], axis=1)
        acc[slot] = alpha * acc[slot] + jnp.dot(probs_bf, values, preferred_element_type=jnp.float32)

    win_blocks = window // rows

    @pl.loop(1, chips + 1)
    def _(step):
        @pl.when(step < chips)
        def _():
            src = lax.rem(chip - step + chips, chips)
            kv_wait(2 * src + core)
            fwd_copy(src).start()

        src = lax.rem(chip - step + 1 + chips, chips)
        kv_wait(2 * src + 1 - core)

        @pl.loop(0, slots)
        def _(slot):
            blk = block_of(slot)
            diagonal = src == blk // 2
            edge = 2 * src <= blk - win_blocks
            inside = (2 * src <= blk) & (2 * src + 1 >= blk - win_blocks)

            @pl.when(inside & jnp.logical_not(diagonal | edge))
            def _():
                attend(slot, src, False)

            @pl.when(inside & (diagonal | edge))
            def _():
                attend(slot, src, True)

    @pl.loop(0, slots)
    def _(slot):
        total = jnp.sum(l_buf[slot], axis=1, keepdims=True)
        obuf[slot] = (acc[slot] / total).astype(jnp.bfloat16)

    def o_copy(slot):
        return pltpu.make_async_remote_copy(obuf.at[slot], out_ref.at[:, lanes(head)], o_send.at[slot], o_recv.at[head],
                                            device_id={'cp': block_of(slot)}, device_id_type=MESH)

    @pl.loop(0, slots)
    def _(slot):
        @pl.when(block_of(slot) != me)
        def _():
            o_copy(slot).start()

        @pl.when(block_of(slot) == me)
        def _():
            pltpu.make_async_copy(obuf.at[slot], out_ref.at[:, lanes(head)], o_recv.at[head]).start()

    @pl.loop(0, n_heads)
    def _(h):
        pltpu.make_async_copy(out_ref.at[:, lanes(h)], out_ref.at[:, lanes(h)], o_recv.at[h]).wait()

        @pl.when(groups * h + my_group != me)
        def _():
            q_copy(h).wait_send()

    @pl.loop(0, slots)
    def _(slot):
        @pl.when(block_of(slot) != me)
        def _():
            o_copy(slot).wait_send()

    @pl.loop(0, chips)
    def _(dst):
        fwd_copy(dst).wait_send()

        @pl.when(dst != chip)
        def _():
            kv_copy(dst).wait_send()


def attention(cp_size, window, collective_id, queries, kv):
    rows, cols = queries.shape
    n_heads = cols // HEAD_DIM
    slots = n_heads
    dma = pltpu.SemaphoreType.DMA
    any_spec = pl.BlockSpec(memory_space=pl.ANY)
    return pl.pallas_call(
        functools.partial(attention_kernel, cp_size, window),
        out_shape=jax.ShapeDtypeStruct((rows, cols), jnp.bfloat16),
        in_specs=[any_spec, any_spec],
        out_specs=any_spec,
        scratch_shapes=[
            pltpu.VMEM((cp_size, 2, rows, HEAD_DIM), jnp.bfloat16),
            pltpu.VMEM((slots, rows, HEAD_DIM), jnp.bfloat16),
            pltpu.VMEM((slots, rows, HEAD_DIM), jnp.bfloat16),
            pltpu.VMEM((slots, rows, HEAD_DIM), jnp.float32),
            pltpu.VMEM((slots, rows, HEAD_DIM), jnp.float32),
            pltpu.VMEM((slots, rows, HEAD_DIM), jnp.float32),
            dma((cp_size // 2,)), dma((cp_size,)), dma((cp_size // 2,)),
            dma((n_heads,)), dma((slots,)), dma((slots,)), dma((n_heads,)),
        ],
        compiler_params=pltpu.CompilerParams(collective_id=collective_id, has_side_effects=True, vmem_limit_bytes=24 * MIB),
        cost_estimate=pl.CostEstimate(flops=4 * 132 * rows * rows * HEAD_DIM, bytes_accessed=8 * MIB, transcendentals=132 * rows * rows),
        name='attention',
    )(queries, kv)


def block_kernel(layer, last, *refs):
    if last:
        (attn_ref, res_ref, gain_ref, wo_ref, wg_ref, wu_ref, wd_ref, out_ref,
         wo_buf, wg_buf, wu_buf, wd_buf, acc, act, sbuf, rbuf, own, gathered, stats, scale_buf,
         wo_sem, gu_sem, wd_sem, rs_send, rs_recv, ag_send, ag_recv, st_send, st_recv, out_sem) = refs
    else:
        (attn_ref, res_ref, gain_ref, wo_ref, wg_ref, wu_ref, wd_ref,
         gain2_ref, cos_ref, sin_ref, wq_ref, bq_ref, wk_ref, bk_ref, wv_ref, bv_ref,
         res_out_ref, q_ref, kv_ref,
         wo_buf, wg_buf, wu_buf, wd_buf, acc, act, sbuf, rbuf, own, gathered, stats, scale_buf,
         wo_sem, gu_sem, wd_sem, rs_send, rs_recv, ag_send, ag_recv, st_send, st_recv,
         wq_buf, wk_buf, wv_buf, qkv_acc, qkv_sem) = refs
    rows, unit = own.shape[1], own.shape[2]
    width = 8 * unit
    ffn = act.shape[1]
    me = lax.axis_index('tp')
    gu_slots, wd_slots = wg_buf.shape[0], wd_buf.shape[0]

    def rs_unit(n):
        pair, odd = n // 2, lax.rem(n, 2)
        mid, first = (pair * (3 - pair)) // 2, (3 - pair) // 3
        half = odd + mid * (2 - pair) * (1 - 2 * odd)
        return 2 * lax.rem(me + 2 * first + mid * (1 + 2 * odd), 4) + half

    def ag_unit(u):
        pair, odd = u // 2, lax.rem(u, 2)
        mid, final = (pair * (3 - pair)) // 2, pair // 3
        half = odd + mid * (pair - 1) * (1 - 2 * odd)
        return 2 * lax.rem(me + mid * (3 - 2 * odd) + 2 * final, 4) + half, mid * (pair - 1 + 2 * odd) + final * (4 + odd)

    def span(idx):
        return pl.ds(pl.multiple_of(idx * unit, unit), unit)

    def wo_copy(n):
        return pltpu.make_async_copy(wo_ref.at[layer, :, span(rs_unit(n))], wo_buf.at[n], wo_sem.at[n])

    def gu_copies(u):
        idx, slot = ag_unit(u)[0], lax.rem(u, gu_slots)
        return (pltpu.make_async_copy(wg_ref.at[layer, :, span(idx)], wg_buf.at[slot], gu_sem.at[0, slot]),
                pltpu.make_async_copy(wu_ref.at[layer, :, span(idx)], wu_buf.at[slot], gu_sem.at[1, slot]))

    def wd_copy(n):
        slot = lax.rem(n, wd_slots)
        return pltpu.make_async_copy(wd_ref.at[layer, :, span(rs_unit(n))], wd_buf.at[slot], wd_sem.at[slot])

    def qkv_copies(u):
        idx, slot = ag_unit(u)[0], lax.rem(u, 2)
        return tuple(pltpu.make_async_copy(w.at[layer + 1, span(idx), :], buf.at[slot], qkv_sem.at[i, slot])
                     for i, (w, buf) in enumerate(((wq_ref, wq_buf), (wk_ref, wk_buf), (wv_ref, wv_buf))))

    def start(copies):
        for copy in copies:
            copy.start()

    def wait(copies):
        for copy in copies:
            copy.wait()

    barrier = pltpu.get_barrier_semaphore()
    for step in (1, 2, 3):
        pl.semaphore_signal(barrier, inc=1, device_id={'tp': lax.rem(me + step, 4)}, device_id_type=MESH)
    pl.loop(0, 8)(lambda n: wo_copy(n).start())
    pl.loop(0, gu_slots)(lambda u: start(gu_copies(u)))
    pl.semaphore_wait(barrier, 3)

    def rs_copy(stage, n):
        return pltpu.make_async_remote_copy(sbuf.at[n], rbuf.at[stage, n], rs_send.at[stage, n], rs_recv.at[stage, n],
                                            device_id={'tp': lax.rem(me + 1 + 2 * lax.rem(n, 2), 4)}, device_id_type=MESH)

    def reduce_scatter(stage, part, after):
        @pl.loop(0, 8)
        def _(n):
            value = part(n)

            @pl.when(n < 4)
            def _():
                sbuf[n] = value.astype(jnp.bfloat16)
                rs_copy(stage, n).start()

            @pl.when((n >= 4) & (n < 6))
            def _():
                rs_copy(stage, n - 4).wait_recv()
                sbuf[n] = (value + rbuf[stage, n - 4].astype(jnp.float32)).astype(jnp.bfloat16)
                rs_copy(stage, n).start()

            @pl.when(n >= 6)
            def _():
                own[n - 6] = value

        after()
        square = jnp.zeros((rows, HEAD_DIM), jnp.float32)
        for half in (0, 1):
            from_left, from_right = (4, 3) if half == 0 else (2, 5)
            rs_copy(stage, from_left).wait_recv()
            rs_copy(stage, from_right).wait_recv()
            residual = res_ref[:, half * unit:(half + 1) * unit] if stage == 0 else gathered[0, 2 * me + half]
            total = own[half] + rbuf[stage, from_left].astype(jnp.float32) + rbuf[stage, from_right].astype(jnp.float32)
            new = (residual.astype(jnp.float32) + total).astype(jnp.bfloat16)
            gathered[stage, 2 * me + half] = new
            new_f = new.astype(jnp.float32)
            for lane in range(0, unit, HEAD_DIM):
                square = square + new_f[:, lane:lane + HEAD_DIM] * new_f[:, lane:lane + HEAD_DIM]
        return square

    def stat_copy(stage, step):
        return pltpu.make_async_remote_copy(stats.at[stage, me], stats.at[stage, me], st_send.at[stage, step - 1], st_recv.at[stage, me],
                                            device_id={'tp': lax.rem(me + step, 4)}, device_id_type=MESH)

    def ag_copy(stage, s):
        if s < 4:
            idx = 2 * me + (0, 1, 1, 0)[s]
        else:
            idx = 2 * lax.rem(me + 3, 4) if s == 4 else 2 * lax.rem(me + 1, 4) + 1
        to = lax.rem(me + (1, 1, 3, 3, 1, 3)[s], 4)
        return pltpu.make_async_remote_copy(gathered.at[stage, idx], gathered.at[stage, idx], ag_send.at[stage, s], ag_recv.at[stage, s],
                                            device_id={'tp': to}, device_id_type=MESH)

    def gather_start(stage, square):
        if square is not None:
            total = jnp.broadcast_to(jnp.sum(square, axis=1, keepdims=True), square.shape)
            stats[stage, me] = jnp.transpose(total)[:8]
            for step in (1, 2, 3):
                stat_copy(stage, step).start()
        for s in (0, 2, 1, 3):
            ag_copy(stage, s).start()
        if square is not None:
            for step in (1, 2, 3):
                source = lax.rem(me + step, 4)
                pltpu.make_async_copy(stats.at[stage, source], stats.at[stage, source], st_recv.at[stage, source]).wait()
            total = stats[stage, 0] + stats[stage, 1] + stats[stage, 2] + stats[stage, 3]
            inverse = lax.rsqrt(total[:1] / width + 1e-6)
            scale_buf[...] = jnp.transpose(jnp.broadcast_to(inverse, (HEAD_DIM, rows)))

    def gather_wait(stage, u):
        idx, sem = ag_unit(u)

        @pl.when(u >= 2)
        def _():
            pltpu.make_async_copy(gathered.at[stage, idx], gathered.at[stage, idx], ag_recv.at[stage, sem]).wait()

        @pl.when(u == 2)
        def _():
            ag_copy(stage, 4).start()

        @pl.when(u == 3)
        def _():
            ag_copy(stage, 5).start()

        return idx

    def finish_sends(stage, with_stats):
        for n in range(6):
            rs_copy(stage, n).wait_send()
            ag_copy(stage, n).wait_send()
        if with_stats:
            for step in (1, 2, 3):
                stat_copy(stage, step).wait_send()

    def normalized(stage, idx, gains):
        raw = gathered[stage, idx].astype(jnp.float32)
        scale = jnp.concatenate([scale_buf[...]] * (unit // HEAD_DIM), axis=1)
        return (raw * scale * gains[idx].astype(jnp.float32)).astype(jnp.bfloat16)

    def accumulate(which, hidden, weight):
        for col in range(0, ffn, 512):
            size = min(512, ffn - col)
            acc[which, col:col + size, :] += lax.dot_general(weight[col:col + size, :], hidden, (((1,), (1,)), ((), ())), preferred_element_type=jnp.float32)

    def out_part(n):
        wo_copy(n).wait()
        return jnp.dot(attn_ref[...], wo_buf[n], preferred_element_type=jnp.float32)

    def before_mlp():
        pl.loop(0, wd_slots)(lambda n: wd_copy(n).start())
        acc[...] = jnp.zeros_like(acc)

    gather_start(0, reduce_scatter(0, out_part, before_mlp))

    @pl.loop(0, 8)
    def _(u):
        idx = gather_wait(0, u)
        hidden = normalized(0, idx, gain_ref)
        wait(gu_copies(u))
        slot = lax.rem(u, gu_slots)
        accumulate(0, hidden, wg_buf.at[slot])
        accumulate(1, hidden, wu_buf.at[slot])

        @pl.when(u + gu_slots < 8)
        def _():
            start(gu_copies(u + gu_slots))

    if not last:
        pl.loop(0, 2)(lambda u: start(qkv_copies(u)))
    for col in range(0, ffn, 256):
        size = min(256, ffn - col)
        gate = acc[0, col:col + 256, :]
        product = gate * lax.logistic(gate) * acc[1, col:col + 256, :]
        act[:, col:col + size] = jnp.transpose(product)[:, :size].astype(jnp.bfloat16)
    finish_sends(0, True)

    def down_part(n):
        wd_copy(n).wait()
        value = jnp.dot(act[...], wd_buf[lax.rem(n, wd_slots)], preferred_element_type=jnp.float32)

        @pl.when(n + wd_slots < 8)
        def _():
            wd_copy(n + wd_slots).start()

        return value

    if last:
        reduce_scatter(1, down_part, lambda: None)
        gather_start(1, None)

        def out_copy(idx):
            return pltpu.make_async_copy(gathered.at[1, idx], out_ref.at[:, span(idx)], out_sem.at[idx])

        pl.loop(0, 8)(lambda u: out_copy(gather_wait(1, u)).start())
        pl.loop(0, 8)(lambda idx: out_copy(idx).wait())
        finish_sends(1, False)
        return

    def before_qkv():
        qkv_acc[...] = jnp.zeros_like(qkv_acc)

    gather_start(1, reduce_scatter(1, down_part, before_qkv))
    cols = q_ref.shape[1]

    @pl.loop(0, 8)
    def _(u):
        idx = gather_wait(1, u)
        hidden = normalized(1, idx, gain2_ref)
        wait(qkv_copies(u))
        slot = lax.rem(u, 2)
        for which, buf in enumerate((wq_buf, wk_buf, wv_buf)):
            for col in range(0, cols, 512):
                part = slice(col, min(col + 512, cols))
                qkv_acc[which, :, part] += jnp.dot(hidden, buf[slot, :, part], preferred_element_type=jnp.float32)

        @pl.when(u + 2 < 8)
        def _():
            start(qkv_copies(u + 2))

    for head in range(0, cols, HEAD_DIM):
        lane = slice(head, head + HEAD_DIM)

        def biased(which, b_ref):
            return qkv_acc[which, :, lane] + b_ref[:, lane].astype(jnp.float32)

        def rope(proj):
            return (proj * cos_ref[...] + pltpu.roll(proj, HEAD_DIM // 2, 1) * sin_ref[...]).astype(jnp.bfloat16)

        q_ref[:, lane] = rope(biased(0, bq_ref))
        kv_ref[0, :, lane] = rope(biased(1, bk_ref))
        kv_ref[1, :, lane] = biased(2, bv_ref).astype(jnp.bfloat16)
    for half in (0, 1):
        res_out_ref[:, half * unit:(half + 1) * unit] = gathered[1, 2 * me + half]
    finish_sends(1, True)


def block(layer, last, collective_id, attn_out, residual, mlp_gain, attn_gain, cos_tab, sin_tab, w_out, w_gate, w_up, w_down,
          w_query, b_query, w_key, b_key, w_value, b_value):
    rows, cols = attn_out.shape
    width, ffn = w_gate.shape[1:]
    unit = width // 8
    bf, f32, dma, vmem = jnp.bfloat16, jnp.float32, pltpu.SemaphoreType.DMA, pltpu.VMEM
    any_spec, vmem_spec = pl.BlockSpec(memory_space=pl.ANY), pl.BlockSpec(memory_space=pltpu.VMEM)
    gu_slots, wd_slots = 2, 3
    gains = lambda table, i: table[i].reshape(8, 1, unit)
    args = [attn_out, residual, gains(mlp_gain, layer), w_out, jnp.swapaxes(w_gate, 1, 2), jnp.swapaxes(w_up, 1, 2), w_down]
    in_specs = [vmem_spec] * 3 + [any_spec] * 4
    scratch = [
        vmem((8, cols, unit), bf), vmem((gu_slots, ffn, unit), bf), vmem((gu_slots, ffn, unit), bf), vmem((wd_slots, ffn, unit), bf),
        vmem((2, -(-ffn // 256) * 256, rows), f32), vmem((rows, ffn), bf), vmem((6, rows, unit), bf), vmem((2, 6, rows, unit), bf),
        vmem((2, rows, unit), f32), vmem((2, 8, rows, unit), bf), vmem((2, 4, 8, rows), f32), vmem((rows, HEAD_DIM), f32),
        dma((8,)), dma((2, gu_slots)), dma((wd_slots,)), dma((2, 6)), dma((2, 6)), dma((2, 6)), dma((2, 6)), dma((2, 3)), dma((2, 4)),
    ]
    if last:
        out_shape, out_specs = jax.ShapeDtypeStruct((rows, width), bf), any_spec
        scratch.append(dma((8,)))
    else:
        nxt = layer + 1
        args += [gains(attn_gain, nxt), cos_tab, sin_tab]
        in_specs += [vmem_spec] * 3
        for w, b in ((w_query, b_query), (w_key, b_key), (w_value, b_value)):
            args += [w, b[nxt:nxt + 1]]
            in_specs += [any_spec, vmem_spec]
        out_shape = (jax.ShapeDtypeStruct((rows, 2 * unit), bf), jax.ShapeDtypeStruct((rows, cols), bf), jax.ShapeDtypeStruct((2, rows, cols), bf))
        out_specs = (vmem_spec,) * 3
        scratch += [vmem((2, unit, cols), bf)] * 3 + [vmem((3, rows, cols), f32), dma((3, 2))]
    return pl.pallas_call(
        functools.partial(block_kernel, layer, last),
        out_shape=out_shape,
        in_specs=in_specs,
        out_specs=out_specs,
        scratch_shapes=scratch,
        compiler_params=pltpu.CompilerParams(collective_id=collective_id, has_side_effects=True, vmem_limit_bytes=63 * MIB),
        cost_estimate=pl.CostEstimate(flops=2 * rows * width * (cols + 3 * ffn), bytes_accessed=2 * width * (cols + 3 * ffn), transcendentals=0),
        name='block',
    )(*args)


def solution(mesh):
    cp_size = mesh.shape['cp']

    def local_step(x_in, positions, attn_gain, mlp_gain, w_query, b_query, w_key, b_key, w_value, b_value, w_out, w_gate, w_up, w_down):
        block_dev, width = x_in.shape
        cos_tab, sin_tab = rope_tables(positions)
        owned = width // 4
        residual = lax.dynamic_slice(x_in, (0, lax.axis_index('tp') * owned), (block_dev, owned))
        queries, kv_full = qkv_project(0, x_in, attn_gain, cos_tab, sin_tab, w_query, b_query, w_key, b_key, w_value, b_value)
        weights = (mlp_gain, attn_gain, cos_tab, sin_tab, w_out, w_gate, w_up, w_down, w_query, b_query, w_key, b_key, w_value, b_value)
        attn_out = attention(cp_size, block_dev * cp_size, 0, queries, kv_full)
        residual, queries, kv_win = block(0, False, 1, attn_out, residual, *weights)
        attn_out = attention(cp_size, WINDOW, 2, queries, kv_win)
        hidden = block(1, True, 3, attn_out, residual, *weights)
        caches = [part.reshape(block_dev, -1, HEAD_DIM) for kv in (kv_full, kv_win) for part in (kv[0], kv[1])]
        return hidden, caches[0], caches[1], caches[2], caches[3]

    weight_col = P(None, None, 'tp')
    bias_col = P(None, 'tp')
    weight_row = P(None, 'tp', None)
    replicated = P(None, None)
    cache_spec = P('cp', 'tp', None)
    in_specs = (P('cp', None), P('cp'), replicated, replicated, weight_col, bias_col, weight_col, bias_col, weight_col, bias_col, weight_row, weight_col, weight_col, weight_row)
    out_specs = (P('cp', None), cache_spec, cache_spec, cache_spec, cache_spec)
    return jax.shard_map(local_step, mesh=mesh, in_specs=in_specs, out_specs=out_specs, check_vma=False)
```

```python
import functools

import jax
import jax.numpy as jnp
from jax import lax
from jax.experimental import pallas as pl
from jax.experimental.pallas import tpu as pltpu
from jax.sharding import PartitionSpec as P

HEAD_DIM = 128
WINDOW = 4096
MESH = pl.DeviceIdType.MESH
NEG = -0.7 * float(jnp.finfo(jnp.float32).max)
LOG2E = 1.4426950408889634
MIB = 1024 * 1024


def rms_norm(hidden, gain):
    hidden_f = hidden.astype(jnp.float32)
    variance = jnp.mean(hidden_f * hidden_f, axis=-1, keepdims=True)
    return (hidden_f * lax.rsqrt(variance + 1e-6) * gain.astype(jnp.float32)).astype(jnp.bfloat16)


def rope_tables(positions):
    inv_freq = 1.0 / (1000000.0 ** (jnp.arange(0, HEAD_DIM, 2, dtype=jnp.float32) / HEAD_DIM))
    angles = positions.astype(jnp.float32)[:, None] * inv_freq[None, :]
    cos, sin = jnp.cos(angles), jnp.sin(angles)
    return jnp.concatenate([cos, cos], axis=-1), jnp.concatenate([-sin, sin], axis=-1)


def qkv_kernel(layer, x_ref, gain_ref, cos_ref, sin_ref, wq_ref, bq_ref, wk_ref, bk_ref, wv_ref, bv_ref, q_ref, kv_ref, normed):
    @pl.when(pl.program_id(0) == 0)
    def _():
        normed[...] = rms_norm(x_ref[...], gain_ref[layer:layer + 1])

    hidden = normed[...]
    cos_tab, sin_tab = cos_ref[...], sin_ref[...]

    def project(w_ref, b_ref):
        return jnp.dot(hidden, w_ref[...], preferred_element_type=jnp.float32) + b_ref[layer:layer + 1].astype(jnp.float32)

    def rope(proj):
        heads = []
        for start in range(0, proj.shape[1], HEAD_DIM):
            head = proj[:, start:start + HEAD_DIM]
            heads.append(head * cos_tab + pltpu.roll(head, HEAD_DIM // 2, 1) * sin_tab)
        return jnp.concatenate(heads, axis=1).astype(jnp.bfloat16)

    q_ref[...] = rope(project(wq_ref, bq_ref))
    kv_ref[0] = rope(project(wk_ref, bk_ref))
    kv_ref[1] = project(wv_ref, bv_ref).astype(jnp.bfloat16)


def qkv_project(layer, hidden, gains, cos_tab, sin_tab, w_query, b_query, w_key, b_key, w_value, b_value, tile=256):
    rows, width = hidden.shape
    cols = w_query.shape[2]
    whole = lambda shape: pl.BlockSpec(shape, lambda n: (0,) * len(shape))
    weight = pl.BlockSpec((None, width, tile), lambda n: (layer, 0, n))
    bias = pl.BlockSpec((2, tile), lambda n: (0, n))
    return pl.pallas_call(
        functools.partial(qkv_kernel, layer),
        grid=(cols // tile,),
        out_shape=(jax.ShapeDtypeStruct((rows, cols), jnp.bfloat16), jax.ShapeDtypeStruct((2, rows, cols), jnp.bfloat16)),
        in_specs=[whole((rows, width)), whole((2, width)), whole(cos_tab.shape), whole(sin_tab.shape), weight, bias, weight, bias, weight, bias],
        out_specs=(pl.BlockSpec((rows, tile), lambda n: (0, n)), pl.BlockSpec((2, rows, tile), lambda n: (0, 0, n))),
        scratch_shapes=[pltpu.VMEM((rows, width), jnp.bfloat16)],
        compiler_params=pltpu.CompilerParams(vmem_limit_bytes=40 * MIB),
        cost_estimate=pl.CostEstimate(flops=6 * rows * width * cols, bytes_accessed=6 * width * cols, transcendentals=0),
        name='qkv',
    )(hidden, gains, cos_tab, sin_tab, w_query, b_query, w_key, b_key, w_value, b_value)


def attention_kernel(cp_size, window, q_ref, kv_ref, out_ref, kvbuf, relay_buf, qbuf, obuf, acc, m_buf, l_buf,
                     kv_send, kv_recv, fwd_send, tie_send, relay_recv, relay_send, q_send, q_recv, o_send, o_recv):
    rows = q_ref.shape[0]
    n_heads = q_ref.shape[1] // HEAD_DIM
    chips = cp_size // 2
    groups = cp_size // n_heads
    slots = cp_size // groups
    me = lax.axis_index('cp')
    chip, core = me // 2, lax.rem(me, 2)
    head, group = me // groups, lax.rem(me, groups)
    sibling = me + 1 - 2 * core
    scale = HEAD_DIM ** -0.5 * LOG2E

    def lanes(h):
        return pl.ds(pl.multiple_of(h * HEAD_DIM, HEAD_DIM), HEAD_DIM)

    def block_of(slot):
        odd = lax.rem(slot, 2)
        return 2 * groups * (slot // 2) + group + odd * (2 * groups - 1 - 2 * group)

    barrier = pltpu.get_barrier_semaphore()

    @pl.loop(1, cp_size)
    def _(step):
        pl.semaphore_signal(barrier, inc=1, device_id={'cp': lax.rem(me + step, cp_size)}, device_id_type=MESH)

    own_kv = pltpu.make_async_copy(kv_ref.at[:, :, lanes(head)], kvbuf.at[me], kv_recv.at[me])
    own_kv.start()
    pl.semaphore_wait(barrier, cp_size - 1)

    place = lax.rem(me, 2 * groups)
    upper = place // groups
    my_group = place + upper * (2 * groups - 1 - 2 * place)
    my_slot = 2 * (me // (2 * groups)) + upper

    def q_copy(h):
        return pltpu.make_async_remote_copy(q_ref.at[:, lanes(h)], qbuf.at[my_slot], q_send.at[h], q_recv.at[my_slot],
                                            device_id={'cp': groups * h + my_group}, device_id_type=MESH)

    def shift(base, dy, dz):
        return 4 * lax.rem(base // 4 + dz, 4) + lax.rem(lax.rem(base, 4) + dy, 4)

    def near(k):
        e = k - 1 + k // 5 + 5 * ((8 - k) // 8)
        return lax.rem(lax.rem(e, 3) + 3, 4), lax.rem(e // 3 + 3, 4)

    def far(j):
        b = j // 4
        rest = b * (j - 4)
        return 2 * (1 - b) + rest + rest // 2, (1 - b) * j + 2 * b

    def first_leg(j):
        way = 1 + 2 * core
        return tuple(d + (d // 2) * (1 - lax.rem(d, 2)) * (way - 2) for d in far(j))

    def source_of(step):
        t = step // 9
        ny, nz = near(step * (1 - t))
        fy, fz = far((step - 9) * t)
        return shift(chip, 4 - (1 - t) * ny - t * fy, 4 - (1 - t) * nz - t * fz)

    def kv_copy(k):
        dst = shift(chip, *near(k))
        return pltpu.make_async_remote_copy(kv_ref.at[:, :, lanes((2 * dst) // groups)], kvbuf.at[me], kv_send.at[k], kv_recv.at[me],
                                            device_id={'cp': 2 * dst + core}, device_id_type=MESH)

    def tie_copy(j):
        dst = shift(chip, *far(j))
        return pltpu.make_async_remote_copy(kv_ref.at[:, :, lanes((2 * dst) // groups)], relay_buf.at[j], tie_send.at[j], relay_recv.at[j],
                                            device_id={'cp': 2 * shift(chip, *first_leg(j)) + core}, device_id_type=MESH)

    def relay_copy(j):
        ly, lz = first_leg(j)
        origin = shift(chip, 4 - ly, 4 - lz)
        blk = 2 * origin + core
        return pltpu.make_async_remote_copy(relay_buf.at[j], kvbuf.at[blk], relay_send.at[j], kv_recv.at[blk],
                                            device_id={'cp': 2 * shift(origin, *far(j)) + core}, device_id_type=MESH)

    def fwd_copy(src):
        blk = 2 * src + core
        return pltpu.make_async_remote_copy(kvbuf.at[blk], kvbuf.at[blk], fwd_send.at[src], kv_recv.at[blk],
                                            device_id={'cp': sibling}, device_id_type=MESH)

    def kv_wait(blk):
        pltpu.make_async_copy(kvbuf.at[blk], kvbuf.at[blk], kv_recv.at[blk]).wait()

    @pl.loop(0, n_heads)
    def _(h):
        @pl.when(groups * h + my_group != me)
        def _():
            q_copy(h).start()

        @pl.when(groups * h + my_group == me)
        def _():
            pltpu.make_async_copy(q_ref.at[:, lanes(h)], qbuf.at[my_slot], q_recv.at[my_slot]).start()

    @pl.loop(1, 9)
    def _(k):
        @pl.when(k < 8)
        def _():
            tie_copy(k - 1).start()

        kv_copy(k).start()

    kv_wait(me)
    fwd_copy(chip).start()

    acc[...] = jnp.zeros_like(acc)
    l_buf[...] = jnp.zeros_like(l_buf)
    m_buf[...] = jnp.full_like(m_buf, NEG)

    @pl.loop(0, slots)
    def _(slot):
        pltpu.make_async_copy(qbuf.at[slot], qbuf.at[slot], q_recv.at[slot]).wait()

    def attend(slot, src, masked):
        keys = kvbuf[pl.ds(2 * src, 2), 0].reshape(2 * rows, HEAD_DIM)
        values = kvbuf[pl.ds(2 * src, 2), 1].reshape(2 * rows, HEAD_DIM)
        scores = lax.dot_general(qbuf[slot], keys, (((1,), (1,)), ((), ())), preferred_element_type=jnp.float32) * scale
        if masked:
            q_pos = block_of(slot) * rows + lax.broadcasted_iota(jnp.int32, scores.shape, 0)
            k_pos = src * 2 * rows + lax.broadcasted_iota(jnp.int32, scores.shape, 1)
            scores = jnp.where((k_pos <= q_pos) & (k_pos > q_pos - window), scores, NEG)
        parts = [scores[:, i:i + HEAD_DIM] for i in range(0, scores.shape[1], HEAD_DIM)] if scores.shape[1] % HEAD_DIM == 0 else [scores]
        m_prev = m_buf[slot]
        m_lane = functools.reduce(jnp.maximum, parts)
        m_new = jnp.maximum(m_prev, jnp.max(m_lane, axis=1, keepdims=True))
        alpha = jnp.exp2(m_prev - m_new)
        probs = [jnp.exp2(part - m_new[:, :part.shape[1]]) for part in parts]
        l_new = functools.reduce(jnp.add, probs)
        if l_new.shape[1] != HEAD_DIM:
            l_new = jnp.concatenate([l_new, jnp.zeros((rows, HEAD_DIM - l_new.shape[1]), jnp.float32)], axis=1)
        l_buf[slot] = alpha * l_buf[slot] + l_new
        m_buf[slot] = m_new
        probs_bf = jnp.concatenate([part.astype(jnp.bfloat16) for part in probs], axis=1)
        acc[slot] = alpha * acc[slot] + jnp.dot(probs_bf, values, preferred_element_type=jnp.float32)

    win_blocks = window // rows

    @pl.loop(1, chips + 1)
    def _(step):
        @pl.when(step < 8)
        def _():
            pltpu.make_async_copy(relay_buf.at[step - 1], relay_buf.at[step - 1], relay_recv.at[step - 1]).wait()
            relay_copy(step - 1).start()

        @pl.when(step < chips)
        def _():
            src = source_of(step)
            kv_wait(2 * src + core)
            fwd_copy(src).start()

        src = source_of(step - 1)
        kv_wait(2 * src + 1 - core)

        @pl.loop(0, slots)
        def _(slot):
            blk = block_of(slot)
            diagonal = src == blk // 2
            edge = 2 * src <= blk - win_blocks
            inside = (2 * src <= blk) & (2 * src + 1 >= blk - win_blocks)

            @pl.when(inside & jnp.logical_not(diagonal | edge))
            def _():
                attend(slot, src, False)

            @pl.when(inside & (diagonal | edge))
            def _():
                attend(slot, src, True)

    @pl.loop(0, slots)
    def _(slot):
        total = jnp.sum(l_buf[slot], axis=1, keepdims=True)
        obuf[slot] = (acc[slot] / total).astype(jnp.bfloat16)

    def o_copy(slot):
        return pltpu.make_async_remote_copy(obuf.at[slot], out_ref.at[:, lanes(head)], o_send.at[slot], o_recv.at[head],
                                            device_id={'cp': block_of(slot)}, device_id_type=MESH)

    @pl.loop(0, slots)
    def _(slot):
        @pl.when(block_of(slot) != me)
        def _():
            o_copy(slot).start()

        @pl.when(block_of(slot) == me)
        def _():
            pltpu.make_async_copy(obuf.at[slot], out_ref.at[:, lanes(head)], o_recv.at[head]).start()

    @pl.loop(0, n_heads)
    def _(h):
        pltpu.make_async_copy(out_ref.at[:, lanes(h)], out_ref.at[:, lanes(h)], o_recv.at[h]).wait()

        @pl.when(groups * h + my_group != me)
        def _():
            q_copy(h).wait_send()

    @pl.loop(0, slots)
    def _(slot):
        @pl.when(block_of(slot) != me)
        def _():
            o_copy(slot).wait_send()

    @pl.loop(0, chips)
    def _(dst):
        fwd_copy(dst).wait_send()

    @pl.loop(1, 9)
    def _(k):
        kv_copy(k).wait_send()

    @pl.loop(0, 7)
    def _(j):
        tie_copy(j).wait_send()
        relay_copy(j).wait_send()


def attention(cp_size, window, collective_id, queries, kv):
    rows, cols = queries.shape
    n_heads = cols // HEAD_DIM
    slots = n_heads
    dma = pltpu.SemaphoreType.DMA
    hbm_spec = pl.BlockSpec(memory_space=pltpu.HBM)
    return pl.pallas_call(
        functools.partial(attention_kernel, cp_size, window),
        out_shape=jax.ShapeDtypeStruct((rows, cols), jnp.bfloat16),
        in_specs=[hbm_spec, hbm_spec],
        out_specs=hbm_spec,
        scratch_shapes=[
            pltpu.VMEM((cp_size, 2, rows, HEAD_DIM), jnp.bfloat16),
            pltpu.VMEM((7, 2, rows, HEAD_DIM), jnp.bfloat16),
            pltpu.VMEM((slots, rows, HEAD_DIM), jnp.bfloat16),
            pltpu.VMEM((slots, rows, HEAD_DIM), jnp.bfloat16),
            pltpu.VMEM((slots, rows, HEAD_DIM), jnp.float32),
            pltpu.VMEM((slots, rows, HEAD_DIM), jnp.float32),
            pltpu.VMEM((slots, rows, HEAD_DIM), jnp.float32),
            dma((9,)), dma((cp_size,)), dma((cp_size // 2,)), dma((7,)), dma((7,)), dma((7,)),
            dma((n_heads,)), dma((slots,)), dma((slots,)), dma((n_heads,)),
        ],
        compiler_params=pltpu.CompilerParams(collective_id=collective_id, has_side_effects=True, vmem_limit_bytes=24 * MIB),
        cost_estimate=pl.CostEstimate(flops=4 * 132 * rows * rows * HEAD_DIM, bytes_accessed=8 * MIB, transcendentals=132 * rows * rows),
        name='attention',
    )(queries, kv)


def block_kernel(layer, last, *refs):
    if last:
        (attn_ref, res_ref, gain_ref, wo_ref, wg_ref, wu_ref, wd_ref, out_ref,
         wo_buf, wg_buf, wu_buf, wd_buf, acc, act, sbuf, rbuf, own, gathered, res_buf, stats, scale_buf,
         res_sem, wo_sem, gu_sem, wd_sem, rs_send, rs_recv, ag_send, ag_recv, st_send, st_recv, out_sem) = refs
    else:
        (attn_ref, res_ref, gain_ref, wo_ref, wg_ref, wu_ref, wd_ref,
         gain2_ref, cos_ref, sin_ref, wq_ref, bq_ref, wk_ref, bk_ref, wv_ref, bv_ref,
         res_out_ref, q_ref, kv_ref,
         wo_buf, wg_buf, wu_buf, wd_buf, acc, act, sbuf, rbuf, own, gathered, res_buf, stats, scale_buf,
         res_sem, wo_sem, gu_sem, wd_sem, rs_send, rs_recv, ag_send, ag_recv, st_send, st_recv,
         wq_buf, wk_buf, wv_buf, qkv_acc, qkv_sem) = refs
    rows, unit = own.shape[1], own.shape[2]
    width = 8 * unit
    ffn = act.shape[1]
    me = lax.axis_index('tp')
    gu_slots, wd_slots = wg_buf.shape[0], wd_buf.shape[0]

    def rs_unit(n):
        pair, odd = n // 2, lax.rem(n, 2)
        mid, first = (pair * (3 - pair)) // 2, (3 - pair) // 3
        half = odd + mid * (2 - pair) * (1 - 2 * odd)
        return 2 * lax.rem(me + 2 * first + mid * (1 + 2 * odd), 4) + half

    def ag_unit(u):
        pair, odd = u // 2, lax.rem(u, 2)
        mid, final = (pair * (3 - pair)) // 2, pair // 3
        half = odd + mid * (pair - 1) * (1 - 2 * odd)
        return 2 * lax.rem(me + mid * (3 - 2 * odd) + 2 * final, 4) + half, mid * (pair - 1 + 2 * odd) + final * (4 + odd)

    def span(idx):
        return pl.ds(pl.multiple_of(idx * unit, unit), unit)

    def wo_copy(n):
        return pltpu.make_async_copy(wo_ref.at[layer, :, span(rs_unit(n))], wo_buf.at[n], wo_sem.at[n])

    def gu_copies(u):
        idx, slot = ag_unit(u)[0], lax.rem(u, gu_slots)
        return (pltpu.make_async_copy(wg_ref.at[layer, :, span(idx)], wg_buf.at[slot], gu_sem.at[0, slot]),
                pltpu.make_async_copy(wu_ref.at[layer, :, span(idx)], wu_buf.at[slot], gu_sem.at[1, slot]))

    def wd_copy(n):
        slot = lax.rem(n, wd_slots)
        return pltpu.make_async_copy(wd_ref.at[layer, :, span(rs_unit(n))], wd_buf.at[slot], wd_sem.at[slot])

    def qkv_copies(u):
        idx, slot = ag_unit(u)[0], lax.rem(u, 2)
        return tuple(pltpu.make_async_copy(w.at[layer + 1, span(idx), :], buf.at[slot], qkv_sem.at[i, slot])
                     for i, (w, buf) in enumerate(((wq_ref, wq_buf), (wk_ref, wk_buf), (wv_ref, wv_buf))))

    def start(copies):
        for copy in copies:
            copy.start()

    def wait(copies):
        for copy in copies:
            copy.wait()

    barrier = pltpu.get_barrier_semaphore()
    for step in (1, 2, 3):
        pl.semaphore_signal(barrier, inc=1, device_id={'tp': lax.rem(me + step, 4)}, device_id_type=MESH)
    first_col = 2 * me * unit if res_ref.shape[1] == width else 0
    res_copy = pltpu.make_async_copy(res_ref.at[:, pl.ds(pl.multiple_of(first_col, unit), 2 * unit)], res_buf, res_sem)
    pl.loop(0, 8)(lambda n: wo_copy(n).start())
    res_copy.start()
    pl.loop(0, gu_slots)(lambda u: start(gu_copies(u)))
    pl.semaphore_wait(barrier, 3)

    def rs_copy(stage, n):
        return pltpu.make_async_remote_copy(sbuf.at[n], rbuf.at[stage, n], rs_send.at[stage, n], rs_recv.at[stage, n],
                                            device_id={'tp': lax.rem(me + 1 + 2 * lax.rem(n, 2), 4)}, device_id_type=MESH)

    def reduce_scatter(stage, part, after):
        @pl.loop(0, 8)
        def _(n):
            value = part(n)

            @pl.when(n < 4)
            def _():
                sbuf[n] = value.astype(jnp.bfloat16)
                rs_copy(stage, n).start()

            @pl.when((n >= 4) & (n < 6))
            def _():
                rs_copy(stage, n - 4).wait_recv()
                sbuf[n] = (value + rbuf[stage, n - 4].astype(jnp.float32)).astype(jnp.bfloat16)
                rs_copy(stage, n).start()

            @pl.when(n >= 6)
            def _():
                own[n - 6] = value

        after()
        square = jnp.zeros((rows, HEAD_DIM), jnp.float32)
        for half in (0, 1):
            from_left, from_right = (4, 3) if half == 0 else (2, 5)
            rs_copy(stage, from_left).wait_recv()
            rs_copy(stage, from_right).wait_recv()
            residual = res_buf[:, half * unit:(half + 1) * unit] if stage == 0 else gathered[0, 2 * me + half]
            total = own[half] + rbuf[stage, from_left].astype(jnp.float32) + rbuf[stage, from_right].astype(jnp.float32)
            new = (residual.astype(jnp.float32) + total).astype(jnp.bfloat16)
            gathered[stage, 2 * me + half] = new
            new_f = new.astype(jnp.float32)
            for lane in range(0, unit, HEAD_DIM):
                square = square + new_f[:, lane:lane + HEAD_DIM] * new_f[:, lane:lane + HEAD_DIM]
        return square

    def stat_copy(stage, step):
        return pltpu.make_async_remote_copy(stats.at[stage, me], stats.at[stage, me], st_send.at[stage, step - 1], st_recv.at[stage, me],
                                            device_id={'tp': lax.rem(me + step, 4)}, device_id_type=MESH)

    def ag_copy(stage, s):
        if s < 4:
            idx = 2 * me + (0, 1, 1, 0)[s]
        else:
            idx = 2 * lax.rem(me + 3, 4) if s == 4 else 2 * lax.rem(me + 1, 4) + 1
        to = lax.rem(me + (1, 1, 3, 3, 1, 3)[s], 4)
        return pltpu.make_async_remote_copy(gathered.at[stage, idx], gathered.at[stage, idx], ag_send.at[stage, s], ag_recv.at[stage, s],
                                            device_id={'tp': to}, device_id_type=MESH)

    def gather_start(stage, square):
        if square is not None:
            total = jnp.broadcast_to(jnp.sum(square, axis=1, keepdims=True), square.shape)
            stats[stage, me] = jnp.transpose(total)[:8]
            for step in (1, 2, 3):
                stat_copy(stage, step).start()
        for s in (0, 2, 1, 3):
            ag_copy(stage, s).start()
        if square is not None:
            for step in (1, 2, 3):
                source = lax.rem(me + step, 4)
                pltpu.make_async_copy(stats.at[stage, source], stats.at[stage, source], st_recv.at[stage, source]).wait()
            total = stats[stage, 0] + stats[stage, 1] + stats[stage, 2] + stats[stage, 3]
            inverse = lax.rsqrt(total[:1] / width + 1e-6)
            scale_buf[...] = jnp.transpose(jnp.broadcast_to(inverse, (HEAD_DIM, rows)))

    def gather_wait(stage, u):
        idx, sem = ag_unit(u)

        @pl.when(u >= 2)
        def _():
            pltpu.make_async_copy(gathered.at[stage, idx], gathered.at[stage, idx], ag_recv.at[stage, sem]).wait()

        @pl.when(u == 2)
        def _():
            ag_copy(stage, 4).start()

        @pl.when(u == 3)
        def _():
            ag_copy(stage, 5).start()

        return idx

    def finish_sends(stage, with_stats):
        for n in range(6):
            rs_copy(stage, n).wait_send()
            ag_copy(stage, n).wait_send()
        if with_stats:
            for step in (1, 2, 3):
                stat_copy(stage, step).wait_send()

    def normalized(stage, idx, gains, row):
        raw = gathered[stage, idx].astype(jnp.float32)
        scale = jnp.concatenate([scale_buf[...]] * (unit // HEAD_DIM), axis=1)
        return (raw * scale * gains[row:row + 1, span(idx)].astype(jnp.float32)).astype(jnp.bfloat16)

    def accumulate(which, hidden, weight):
        for col in range(0, ffn, 512):
            size = min(512, ffn - col)
            acc[which, col:col + size, :] += lax.dot_general(weight[col:col + size, :], hidden, (((1,), (1,)), ((), ())), preferred_element_type=jnp.float32)

    def out_part(n):
        wo_copy(n).wait()
        return jnp.dot(attn_ref[...], wo_buf[n], preferred_element_type=jnp.float32)

    def before_mlp():
        pl.loop(0, wd_slots)(lambda n: wd_copy(n).start())
        acc[...] = jnp.zeros_like(acc)
        res_copy.wait()

    gather_start(0, reduce_scatter(0, out_part, before_mlp))

    @pl.loop(0, 8)
    def _(u):
        idx = gather_wait(0, u)
        hidden = normalized(0, idx, gain_ref, layer)
        wait(gu_copies(u))
        slot = lax.rem(u, gu_slots)
        accumulate(0, hidden, wg_buf.at[slot])
        accumulate(1, hidden, wu_buf.at[slot])

        @pl.when(u + gu_slots < 8)
        def _():
            start(gu_copies(u + gu_slots))

    if not last:
        pl.loop(0, 2)(lambda u: start(qkv_copies(u)))
    for col in range(0, ffn, 256):
        size = min(256, ffn - col)
        gate = acc[0, col:col + 256, :]
        product = gate * lax.logistic(gate) * acc[1, col:col + 256, :]
        act[:, col:col + size] = jnp.transpose(product)[:, :size].astype(jnp.bfloat16)
    finish_sends(0, True)

    def down_part(n):
        wd_copy(n).wait()
        value = jnp.dot(act[...], wd_buf[lax.rem(n, wd_slots)], preferred_element_type=jnp.float32)

        @pl.when(n + wd_slots < 8)
        def _():
            wd_copy(n + wd_slots).start()

        return value

    if last:
        reduce_scatter(1, down_part, lambda: None)
        gather_start(1, None)

        def out_copy(idx):
            return pltpu.make_async_copy(gathered.at[1, idx], out_ref.at[:, span(idx)], out_sem.at[idx])

        pl.loop(0, 8)(lambda u: out_copy(gather_wait(1, u)).start())
        pl.loop(0, 8)(lambda idx: out_copy(idx).wait())
        finish_sends(1, False)
        return

    def before_qkv():
        qkv_acc[...] = jnp.zeros_like(qkv_acc)

    gather_start(1, reduce_scatter(1, down_part, before_qkv))
    cols = q_ref.shape[1]

    @pl.loop(0, 8)
    def _(u):
        idx = gather_wait(1, u)
        hidden = normalized(1, idx, gain2_ref, layer + 1)
        wait(qkv_copies(u))
        slot = lax.rem(u, 2)
        for which, buf in enumerate((wq_buf, wk_buf, wv_buf)):
            for col in range(0, cols, 512):
                part = slice(col, min(col + 512, cols))
                qkv_acc[which, :, part] += jnp.dot(hidden, buf[slot, :, part], preferred_element_type=jnp.float32)

        @pl.when(u + 2 < 8)
        def _():
            start(qkv_copies(u + 2))

    for head in range(0, cols, HEAD_DIM):
        lane = slice(head, head + HEAD_DIM)

        def biased(which, b_ref):
            return qkv_acc[which, :, lane] + b_ref[layer + 1:layer + 2, lane].astype(jnp.float32)

        def rope(proj):
            return (proj * cos_ref[...] + pltpu.roll(proj, HEAD_DIM // 2, 1) * sin_ref[...]).astype(jnp.bfloat16)

        q_ref[:, lane] = rope(biased(0, bq_ref))
        kv_ref[0, :, lane] = rope(biased(1, bk_ref))
        kv_ref[1, :, lane] = biased(2, bv_ref).astype(jnp.bfloat16)
    for half in (0, 1):
        res_out_ref[:, half * unit:(half + 1) * unit] = gathered[1, 2 * me + half]
    finish_sends(1, True)


def block(layer, last, collective_id, attn_out, residual, mlp_gain, attn_gain, cos_tab, sin_tab, w_out, w_gate, w_up, w_down,
          w_query, b_query, w_key, b_key, w_value, b_value):
    rows, cols = attn_out.shape
    width, ffn = w_gate.shape[1:]
    unit = width // 8
    bf, f32, dma, vmem = jnp.bfloat16, jnp.float32, pltpu.SemaphoreType.DMA, pltpu.VMEM
    any_spec, vmem_spec = pl.BlockSpec(memory_space=pl.ANY), pl.BlockSpec(memory_space=pltpu.VMEM)
    gu_slots, wd_slots = 2, 3
    args = [attn_out, residual, mlp_gain, w_out, jnp.swapaxes(w_gate, 1, 2), jnp.swapaxes(w_up, 1, 2), w_down]
    in_specs = [vmem_spec, any_spec, vmem_spec] + [any_spec] * 4
    scratch = [
        vmem((8, cols, unit), bf), vmem((gu_slots, ffn, unit), bf), vmem((gu_slots, ffn, unit), bf), vmem((wd_slots, ffn, unit), bf),
        vmem((2, -(-ffn // 256) * 256, rows), f32), vmem((rows, ffn), bf), vmem((6, rows, unit), bf), vmem((2, 6, rows, unit), bf),
        vmem((2, rows, unit), f32), vmem((2, 8, rows, unit), bf), vmem((rows, 2 * unit), bf), vmem((2, 4, 8, rows), f32), vmem((rows, HEAD_DIM), f32),
        dma(()), dma((8,)), dma((2, gu_slots)), dma((wd_slots,)), dma((2, 6)), dma((2, 6)), dma((2, 6)), dma((2, 6)), dma((2, 3)), dma((2, 4)),
    ]
    if last:
        out_shape, out_specs = jax.ShapeDtypeStruct((rows, width), bf), any_spec
        scratch.append(dma((8,)))
    else:
        args += [attn_gain, cos_tab, sin_tab]
        in_specs += [vmem_spec] * 3
        for w, b in ((w_query, b_query), (w_key, b_key), (w_value, b_value)):
            args += [w, b]
            in_specs += [any_spec, vmem_spec]
        out_shape = (jax.ShapeDtypeStruct((rows, 2 * unit), bf), jax.ShapeDtypeStruct((rows, cols), bf), jax.ShapeDtypeStruct((2, rows, cols), bf))
        out_specs = (vmem_spec,) * 3
        scratch += [vmem((2, unit, cols), bf)] * 3 + [vmem((3, rows, cols), f32), dma((3, 2))]
    return pl.pallas_call(
        functools.partial(block_kernel, layer, last),
        out_shape=out_shape,
        in_specs=in_specs,
        out_specs=out_specs,
        scratch_shapes=scratch,
        compiler_params=pltpu.CompilerParams(collective_id=collective_id, has_side_effects=True, vmem_limit_bytes=63 * MIB),
        cost_estimate=pl.CostEstimate(flops=2 * rows * width * (cols + 3 * ffn), bytes_accessed=2 * width * (cols + 3 * ffn), transcendentals=0),
        name='block',
    )(*args)


def solution(mesh):
    cp_size = mesh.shape['cp']

    def local_step(x_in, positions, attn_gain, mlp_gain, w_query, b_query, w_key, b_key, w_value, b_value, w_out, w_gate, w_up, w_down):
        block_dev = x_in.shape[0]
        cos_tab, sin_tab = rope_tables(positions)
        queries, kv_full = qkv_project(0, x_in, attn_gain, cos_tab, sin_tab, w_query, b_query, w_key, b_key, w_value, b_value)
        weights = (mlp_gain, attn_gain, cos_tab, sin_tab, w_out, w_gate, w_up, w_down, w_query, b_query, w_key, b_key, w_value, b_value)
        attn_out = attention(cp_size, block_dev * cp_size, 0, queries, kv_full)
        residual, queries, kv_win = block(0, False, 1, attn_out, x_in, *weights)
        attn_out = attention(cp_size, WINDOW, 2, queries, kv_win)
        hidden = block(1, True, 3, attn_out, residual, *weights)
        caches = [part.reshape(block_dev, -1, HEAD_DIM) for kv in (kv_full, kv_win) for part in (kv[0], kv[1])]
        return hidden, caches[0], caches[1], caches[2], caches[3]

    weight_col = P(None, None, 'tp')
    bias_col = P(None, 'tp')
    weight_row = P(None, 'tp', None)
    replicated = P(None, None)
    cache_spec = P('cp', 'tp', None)
    in_specs = (P('cp', None), P('cp'), replicated, replicated, weight_col, bias_col, weight_col, bias_col, weight_col, bias_col, weight_row, weight_col, weight_col, weight_row)
    out_specs = (P('cp', None), cache_spec, cache_spec, cache_spec, cache_spec)
    return jax.shard_map(local_step, mesh=mesh, in_specs=in_specs, out_specs=out_specs, check_vma=False)
```

```python
import functools

import jax
import jax.numpy as jnp
from jax import lax
from jax.experimental import pallas as pl
from jax.experimental.pallas import tpu as pltpu
from jax.sharding import PartitionSpec as P

HEAD_DIM = 128
WINDOW = 4096
MESH = pl.DeviceIdType.MESH
NEG = -0.7 * float(jnp.finfo(jnp.float32).max)
OTHERS = (1, 2, 3)
LOG2E = 1.4426950408889634
MIB = 1024 * 1024


def rms_norm(hidden, gain):
    hidden_f = hidden.astype(jnp.float32)
    variance = jnp.mean(hidden_f * hidden_f, axis=-1, keepdims=True)
    return (hidden_f * lax.rsqrt(variance + 1e-6) * gain.astype(jnp.float32)).astype(jnp.bfloat16)


def rope_tables(positions):
    inv_freq = 1.0 / (1000000.0 ** (jnp.arange(0, HEAD_DIM, 2, dtype=jnp.float32) / HEAD_DIM))
    angles = positions.astype(jnp.float32)[:, None] * inv_freq[None, :]
    cos, sin = jnp.cos(angles), jnp.sin(angles)
    return jnp.concatenate([cos, cos], axis=-1), jnp.concatenate([-sin, sin], axis=-1)


def qkv_kernel(layer, x_ref, gain_ref, cos_ref, sin_ref, wq_ref, bq_ref, wk_ref, bk_ref, wv_ref, bv_ref, q_ref, kv_ref, normed):
    @pl.when(pl.program_id(0) == 0)
    def _():
        normed[...] = rms_norm(x_ref[...], gain_ref[layer:layer + 1])

    hidden = normed[...]
    cos_tab, sin_tab = cos_ref[...], sin_ref[...]

    def project(w_ref, b_ref):
        return jnp.dot(hidden, w_ref[...], preferred_element_type=jnp.float32) + b_ref[layer:layer + 1].astype(jnp.float32)

    def rope(proj):
        heads = []
        for start in range(0, proj.shape[1], HEAD_DIM):
            head = proj[:, start:start + HEAD_DIM]
            heads.append(head * cos_tab + pltpu.roll(head, HEAD_DIM // 2, 1) * sin_tab)
        return jnp.concatenate(heads, axis=1).astype(jnp.bfloat16)

    q_ref[...] = rope(project(wq_ref, bq_ref))
    kv_ref[0] = rope(project(wk_ref, bk_ref))
    kv_ref[1] = project(wv_ref, bv_ref).astype(jnp.bfloat16)


def qkv_project(layer, hidden, gains, cos_tab, sin_tab, w_query, b_query, w_key, b_key, w_value, b_value, tile=256):
    rows, width = hidden.shape
    cols = w_query.shape[2]
    whole = lambda shape: pl.BlockSpec(shape, lambda n: (0,) * len(shape))
    weight = pl.BlockSpec((None, width, tile), lambda n: (layer, 0, n))
    bias = pl.BlockSpec((2, tile), lambda n: (0, n))
    return pl.pallas_call(
        functools.partial(qkv_kernel, layer),
        grid=(cols // tile,),
        out_shape=(jax.ShapeDtypeStruct((rows, cols), jnp.bfloat16), jax.ShapeDtypeStruct((2, rows, cols), jnp.bfloat16)),
        in_specs=[whole((rows, width)), whole((2, width)), whole(cos_tab.shape), whole(sin_tab.shape), weight, bias, weight, bias, weight, bias],
        out_specs=(pl.BlockSpec((rows, tile), lambda n: (0, n)), pl.BlockSpec((2, rows, tile), lambda n: (0, 0, n))),
        scratch_shapes=[pltpu.VMEM((rows, width), jnp.bfloat16)],
        compiler_params=pltpu.CompilerParams(vmem_limit_bytes=40 * MIB),
        cost_estimate=pl.CostEstimate(flops=6 * rows * width * cols, bytes_accessed=6 * width * cols, transcendentals=0),
        name='qkv',
    )(hidden, gains, cos_tab, sin_tab, w_query, b_query, w_key, b_key, w_value, b_value)


def attention_kernel(cp_size, window, q_ref, kv_ref, out_ref, kvbuf, relay_buf, qbuf, obuf, acc, m_buf, l_buf,
                     kv_send, kv_recv, fwd_send, tie_send, relay_recv, relay_send, q_send, q_recv, o_send, o_recv):
    rows = q_ref.shape[0]
    n_heads = q_ref.shape[1] // HEAD_DIM
    chips = cp_size // 2
    groups = cp_size // n_heads
    slots = cp_size // groups
    me = lax.axis_index('cp')
    chip, core = me // 2, lax.rem(me, 2)
    head, group = me // groups, lax.rem(me, groups)
    sibling = me + 1 - 2 * core
    scale = HEAD_DIM ** -0.5 * LOG2E

    def lanes(h):
        return pl.ds(pl.multiple_of(h * HEAD_DIM, HEAD_DIM), HEAD_DIM)

    def block_of(slot):
        odd = lax.rem(slot, 2)
        return 2 * groups * (slot // 2) + group + odd * (2 * groups - 1 - 2 * group)

    barrier = pltpu.get_barrier_semaphore()

    @pl.loop(1, cp_size)
    def _(step):
        pl.semaphore_signal(barrier, inc=1, device_id={'cp': lax.rem(me + step, cp_size)}, device_id_type=MESH)

    own_kv = pltpu.make_async_copy(kv_ref.at[:, :, lanes(head)], kvbuf.at[me], kv_recv.at[me])
    own_kv.start()
    pl.semaphore_wait(barrier, cp_size - 1)

    place = lax.rem(me, 2 * groups)
    upper = place // groups
    my_group = place + upper * (2 * groups - 1 - 2 * place)
    my_slot = 2 * (me // (2 * groups)) + upper

    def q_copy(h):
        return pltpu.make_async_remote_copy(q_ref.at[:, lanes(h)], qbuf.at[my_slot], q_send.at[h], q_recv.at[my_slot],
                                            device_id={'cp': groups * h + my_group}, device_id_type=MESH)

    def shift(base, dy, dz):
        return 4 * lax.rem(base // 4 + dz, 4) + lax.rem(lax.rem(base, 4) + dy, 4)

    def near(k):
        e = k - 1 + k // 5 + 5 * ((8 - k) // 8)
        return lax.rem(lax.rem(e, 3) + 3, 4), lax.rem(e // 3 + 3, 4)

    def far(j):
        b = j // 4
        rest = b * (j - 4)
        return 2 * (1 - b) + rest + rest // 2, (1 - b) * j + 2 * b

    def first_leg(j):
        way = 1 + 2 * core
        return tuple(d + (d // 2) * (1 - lax.rem(d, 2)) * (way - 2) for d in far(j))

    def source_of(step):
        late = (step + 13) // 16
        t = lax.rem(step, 2) * late
        fresh = (step + 15) // 16
        ny, nz = near((step // 2 + fresh) * (1 - t))
        fy, fz = far((step - 3) // 2 * t)
        return shift(chip, 4 - (1 - t) * ny - t * fy, 4 - (1 - t) * nz - t * fz)

    def kv_copy(k):
        dst = shift(chip, *near(k))
        return pltpu.make_async_remote_copy(kv_ref.at[:, :, lanes((2 * dst) // groups)], kvbuf.at[me], kv_send.at[k], kv_recv.at[me],
                                            device_id={'cp': 2 * dst + core}, device_id_type=MESH)

    def tie_copy(j):
        dst = shift(chip, *far(j))
        return pltpu.make_async_remote_copy(kv_ref.at[:, :, lanes((2 * dst) // groups)], relay_buf.at[j], tie_send.at[j], relay_recv.at[j],
                                            device_id={'cp': 2 * shift(chip, *first_leg(j)) + core}, device_id_type=MESH)

    def relay_copy(j):
        ly, lz = first_leg(j)
        origin = shift(chip, 4 - ly, 4 - lz)
        blk = 2 * origin + core
        return pltpu.make_async_remote_copy(relay_buf.at[j], kvbuf.at[blk], relay_send.at[j], kv_recv.at[blk],
                                            device_id={'cp': 2 * shift(origin, *far(j)) + core}, device_id_type=MESH)

    def fwd_copy(src):
        blk = 2 * src + core
        return pltpu.make_async_remote_copy(kvbuf.at[blk], kvbuf.at[blk], fwd_send.at[src], kv_recv.at[blk],
                                            device_id={'cp': sibling}, device_id_type=MESH)

    def kv_wait(blk):
        pltpu.make_async_copy(kvbuf.at[blk], kvbuf.at[blk], kv_recv.at[blk]).wait()

    @pl.loop(0, n_heads)
    def _(h):
        @pl.when(groups * h + my_group != me)
        def _():
            q_copy(h).start()

        @pl.when(groups * h + my_group == me)
        def _():
            pltpu.make_async_copy(q_ref.at[:, lanes(h)], qbuf.at[my_slot], q_recv.at[my_slot]).start()

    @pl.loop(0, 3)
    def _(k):
        @pl.when(k < 2)
        def _():
            tie_copy(k).start()

        kv_copy(k + 1).start()

    kv_wait(me)
    fwd_copy(chip).start()

    acc[...] = jnp.zeros_like(acc)
    l_buf[...] = jnp.zeros_like(l_buf)
    m_buf[...] = jnp.full_like(m_buf, NEG)

    @pl.loop(0, slots)
    def _(slot):
        pltpu.make_async_copy(qbuf.at[slot], qbuf.at[slot], q_recv.at[slot]).wait()

    def attend(slot, src, masked):
        keys = kvbuf[pl.ds(2 * src, 2), 0].reshape(2 * rows, HEAD_DIM)
        values = kvbuf[pl.ds(2 * src, 2), 1].reshape(2 * rows, HEAD_DIM)
        scores = lax.dot_general(qbuf[slot], keys, (((1,), (1,)), ((), ())), preferred_element_type=jnp.float32) * scale
        if masked:
            q_pos = block_of(slot) * rows + lax.broadcasted_iota(jnp.int32, scores.shape, 0)
            k_pos = src * 2 * rows + lax.broadcasted_iota(jnp.int32, scores.shape, 1)
            scores = jnp.where((k_pos <= q_pos) & (k_pos > q_pos - window), scores, NEG)
        parts = [scores[:, i:i + HEAD_DIM] for i in range(0, scores.shape[1], HEAD_DIM)]
        m_prev = m_buf[slot]
        m_lane = functools.reduce(jnp.maximum, parts)
        m_new = jnp.maximum(m_prev, jnp.max(m_lane, axis=1, keepdims=True))
        alpha = jnp.exp2(m_prev - m_new)
        probs = [jnp.exp2(part - m_new) for part in parts]
        l_new = functools.reduce(jnp.add, probs)
        l_buf[slot] = alpha * l_buf[slot] + l_new
        m_buf[slot] = m_new
        probs_bf = jnp.concatenate([part.astype(jnp.bfloat16) for part in probs], axis=1)
        acc[slot] = alpha * acc[slot] + jnp.dot(probs_bf, values, preferred_element_type=jnp.float32)

    win_blocks = window // rows

    @pl.loop(1, chips + 1)
    def _(step):
        half = step // 2

        @pl.when((lax.rem(step, 2) == 1) & (step < 14))
        def _():
            pltpu.make_async_copy(relay_buf.at[half], relay_buf.at[half], relay_recv.at[half]).wait()
            relay_copy(half).start()

            @pl.when(half < 5)
            def _():
                tie_copy(half).wait_send()
                tie_copy(half + 2).start()

        @pl.when((lax.rem(step, 2) == 0) & (half < 6))
        def _():
            kv_copy(half).wait_send()
            kv_copy(half + 3).start()

        @pl.when(step < chips)
        def _():
            src = source_of(step)
            kv_wait(2 * src + core)
            fwd_copy(src).start()

        src = source_of(step - 1)
        kv_wait(2 * src + 1 - core)

        @pl.loop(0, slots // 2)
        def _(pair):
            low, high = block_of(2 * pair), block_of(2 * pair + 1)
            clean = (src < low // 2) & (2 * src > high - win_blocks)

            @pl.when(clean)
            def _():
                attend(2 * pair, src, False)
                attend(2 * pair + 1, src, False)

            @pl.when(jnp.logical_not(clean))
            def _():
                @pl.loop(2 * pair, 2 * pair + 2)
                def _(slot):
                    blk = block_of(slot)

                    @pl.when((2 * src <= blk) & (2 * src + 1 >= blk - win_blocks))
                    def _():
                        attend(slot, src, True)

    @pl.loop(0, slots)
    def _(slot):
        total = jnp.sum(l_buf[slot], axis=1, keepdims=True)
        obuf[slot] = (acc[slot] / total).astype(jnp.bfloat16)

    def o_copy(slot):
        return pltpu.make_async_remote_copy(obuf.at[slot], out_ref.at[:, lanes(head)], o_send.at[slot], o_recv.at[head],
                                            device_id={'cp': block_of(slot)}, device_id_type=MESH)

    @pl.loop(0, slots)
    def _(slot):
        @pl.when(block_of(slot) != me)
        def _():
            o_copy(slot).start()

        @pl.when(block_of(slot) == me)
        def _():
            pltpu.make_async_copy(obuf.at[slot], out_ref.at[:, lanes(head)], o_recv.at[head]).start()

    @pl.loop(0, n_heads)
    def _(h):
        pltpu.make_async_copy(out_ref.at[:, lanes(h)], out_ref.at[:, lanes(h)], o_recv.at[h]).wait()

        @pl.when(groups * h + my_group != me)
        def _():
            q_copy(h).wait_send()

    @pl.loop(0, slots)
    def _(slot):
        @pl.when(block_of(slot) != me)
        def _():
            o_copy(slot).wait_send()

    @pl.loop(0, chips)
    def _(dst):
        fwd_copy(dst).wait_send()

    @pl.loop(6, 9)
    def _(k):
        kv_copy(k).wait_send()

    @pl.loop(0, 7)
    def _(j):
        @pl.when(j >= 5)
        def _():
            tie_copy(j).wait_send()

        relay_copy(j).wait_send()


def attention(cp_size, window, collective_id, queries, kv):
    rows, cols = queries.shape
    n_heads = cols // HEAD_DIM
    slots = n_heads
    dma = pltpu.SemaphoreType.DMA
    hbm_spec = pl.BlockSpec(memory_space=pltpu.HBM)
    return pl.pallas_call(
        functools.partial(attention_kernel, cp_size, window),
        out_shape=jax.ShapeDtypeStruct((rows, cols), jnp.bfloat16),
        in_specs=[hbm_spec, hbm_spec],
        out_specs=hbm_spec,
        scratch_shapes=[
            pltpu.VMEM((cp_size, 2, rows, HEAD_DIM), jnp.bfloat16),
            pltpu.VMEM((7, 2, rows, HEAD_DIM), jnp.bfloat16),
            pltpu.VMEM((slots, rows, HEAD_DIM), jnp.bfloat16),
            pltpu.VMEM((slots, rows, HEAD_DIM), jnp.bfloat16),
            pltpu.VMEM((slots, rows, HEAD_DIM), jnp.float32),
            pltpu.VMEM((slots, rows, HEAD_DIM), jnp.float32),
            pltpu.VMEM((slots, rows, HEAD_DIM), jnp.float32),
            dma((9,)), dma((cp_size,)), dma((cp_size // 2,)), dma((7,)), dma((7,)), dma((7,)),
            dma((n_heads,)), dma((slots,)), dma((slots,)), dma((n_heads,)),
        ],
        compiler_params=pltpu.CompilerParams(collective_id=collective_id, has_side_effects=True, vmem_limit_bytes=24 * MIB),
        cost_estimate=pl.CostEstimate(flops=4 * 132 * rows * rows * HEAD_DIM, bytes_accessed=8 * MIB, transcendentals=132 * rows * rows),
        name='attention',
    )(queries, kv)


def block_kernel(layer, last, *refs):
    if last:
        (attn_ref, res_ref, gain_ref, wo_ref, wg_ref, wu_ref, wd_ref, out_ref,
         wo_buf, wg_buf, wu_buf, wd_buf, acc, act, sbuf, rbuf, own, gathered, res_buf, stats, scale_buf,
         res_sem, wo_sem, gu_sem, wd_sem, rs_send, rs_recv, ag_send, ag_recv, st_send, st_recv, out_sem) = refs
    else:
        (attn_ref, res_ref, gain_ref, wo_ref, wg_ref, wu_ref, wd_ref,
         gain2_ref, cos_ref, sin_ref, wq_ref, bq_ref, wk_ref, bk_ref, wv_ref, bv_ref,
         res_out_ref, q_ref, kv_ref,
         wo_buf, wg_buf, wu_buf, wd_buf, acc, act, sbuf, rbuf, own, gathered, res_buf, stats, scale_buf,
         res_sem, wo_sem, gu_sem, wd_sem, rs_send, rs_recv, ag_send, ag_recv, st_send, st_recv,
         wq_buf, wk_buf, wv_buf, qkv_acc, qkv_sem) = refs
    rows, unit = own.shape[1], own.shape[2]
    width = 8 * unit
    ffn = act.shape[1]
    me = lax.axis_index('tp')
    gu_slots, wd_slots = wg_buf.shape[0], wd_buf.shape[0]

    def rs_unit(n):
        pair, odd = n // 2, lax.rem(n, 2)
        mid, first = (pair * (3 - pair)) // 2, (3 - pair) // 3
        half = odd + mid * (2 - pair) * (1 - 2 * odd)
        return 2 * lax.rem(me + 2 * first + mid * (1 + 2 * odd), 4) + half

    def ag_unit(u):
        pair, odd = u // 2, lax.rem(u, 2)
        mid, final = (pair * (3 - pair)) // 2, pair // 3
        half = odd + mid * (pair - 1) * (1 - 2 * odd)
        return 2 * lax.rem(me + mid * (3 - 2 * odd) + 2 * final, 4) + half, mid * (pair - 1 + 2 * odd) + final * (4 + odd)

    def span(idx):
        return pl.ds(pl.multiple_of(idx * unit, unit), unit)

    def wo_copy(n):
        return pltpu.make_async_copy(wo_ref.at[layer, :, span(rs_unit(n))], wo_buf.at[n], wo_sem.at[n])

    def gu_copies(u):
        idx, slot = ag_unit(u)[0], lax.rem(u, gu_slots)
        return (pltpu.make_async_copy(wg_ref.at[layer, :, span(idx)], wg_buf.at[slot], gu_sem.at[0, slot]),
                pltpu.make_async_copy(wu_ref.at[layer, :, span(idx)], wu_buf.at[slot], gu_sem.at[1, slot]))

    def wd_copy(n):
        slot = lax.rem(n, wd_slots)
        return pltpu.make_async_copy(wd_ref.at[layer, :, span(rs_unit(n))], wd_buf.at[slot], wd_sem.at[slot])

    def qkv_copies(u):
        idx, slot = ag_unit(u)[0], lax.rem(u, 2)
        return tuple(pltpu.make_async_copy(w.at[layer + 1, span(idx), :], buf.at[slot], qkv_sem.at[i, slot])
                     for i, (w, buf) in enumerate(((wq_ref, wq_buf), (wk_ref, wk_buf), (wv_ref, wv_buf))))

    def start(copies):
        for copy in copies:
            copy.start()

    def wait(copies):
        for copy in copies:
            copy.wait()

    barrier = pltpu.get_barrier_semaphore()
    for step in OTHERS:
        pl.semaphore_signal(barrier, inc=1, device_id={'tp': lax.rem(me + step, 4)}, device_id_type=MESH)
    first_col = 2 * me * unit if res_ref.shape[1] == width else 0
    res_copy = pltpu.make_async_copy(res_ref.at[:, pl.ds(pl.multiple_of(first_col, unit), 2 * unit)], res_buf, res_sem)
    pl.loop(0, 8)(lambda n: wo_copy(n).start())
    res_copy.start()
    pl.loop(0, gu_slots)(lambda u: start(gu_copies(u)))
    pl.semaphore_wait(barrier, 3)

    def rs_copy(stage, n):
        return pltpu.make_async_remote_copy(sbuf.at[n], rbuf.at[stage, n], rs_send.at[stage, n], rs_recv.at[stage, n],
                                            device_id={'tp': lax.rem(me + 1 + 2 * lax.rem(n, 2), 4)}, device_id_type=MESH)

    def reduce_scatter(stage, part, after):
        @pl.loop(0, 8)
        def _(n):
            value = part(n)

            @pl.when(n < 4)
            def _():
                sbuf[n] = value.astype(jnp.bfloat16)
                rs_copy(stage, n).start()

            @pl.when((n >= 4) & (n < 6))
            def _():
                rs_copy(stage, n - 4).wait_recv()
                sbuf[n] = (value + rbuf[stage, n - 4].astype(jnp.float32)).astype(jnp.bfloat16)
                rs_copy(stage, n).start()

            @pl.when(n >= 6)
            def _():
                own[n - 6] = value

        after()
        square = jnp.zeros((rows, HEAD_DIM), jnp.float32)
        for half in (0, 1):
            from_left, from_right = (4, 3) if half == 0 else (2, 5)
            rs_copy(stage, from_left).wait_recv()
            rs_copy(stage, from_right).wait_recv()
            residual = res_buf[:, half * unit:(half + 1) * unit] if stage == 0 else gathered[0, 2 * me + half]
            total = own[half] + rbuf[stage, from_left].astype(jnp.float32) + rbuf[stage, from_right].astype(jnp.float32)
            new = (residual.astype(jnp.float32) + total).astype(jnp.bfloat16)
            gathered[stage, 2 * me + half] = new
            new_f = new.astype(jnp.float32)
            for lane in range(0, unit, HEAD_DIM):
                square = square + new_f[:, lane:lane + HEAD_DIM] * new_f[:, lane:lane + HEAD_DIM]
        return square

    def stat_copy(stage, step):
        return pltpu.make_async_remote_copy(stats.at[stage, me], stats.at[stage, me], st_send.at[stage, step - 1], st_recv.at[stage, me],
                                            device_id={'tp': lax.rem(me + step, 4)}, device_id_type=MESH)

    def ag_copy(stage, s):
        if s < 4:
            idx = 2 * me + (0, 1, 1, 0)[s]
        else:
            idx = 2 * lax.rem(me + 3, 4) if s == 4 else 2 * lax.rem(me + 1, 4) + 1
        to = lax.rem(me + (1, 1, 3, 3, 1, 3)[s], 4)
        return pltpu.make_async_remote_copy(gathered.at[stage, idx], gathered.at[stage, idx], ag_send.at[stage, s], ag_recv.at[stage, s],
                                            device_id={'tp': to}, device_id_type=MESH)

    def gather_start(stage, square):
        if square is not None:
            total = jnp.broadcast_to(jnp.sum(square, axis=1, keepdims=True), square.shape)
            stats[stage, me] = jnp.transpose(total)[:8]
            for step in OTHERS:
                stat_copy(stage, step).start()
        for s in (0, 2, 1, 3):
            ag_copy(stage, s).start()
        if square is not None:
            for step in OTHERS:
                source = lax.rem(me + step, 4)
                pltpu.make_async_copy(stats.at[stage, source], stats.at[stage, source], st_recv.at[stage, source]).wait()
            total = stats[stage, 0] + stats[stage, 1] + stats[stage, 2] + stats[stage, 3]
            inverse = lax.rsqrt(total[:1] / width + 1e-6)
            scale_buf[...] = jnp.transpose(jnp.broadcast_to(inverse, (HEAD_DIM, rows)))

    def gather_wait(stage, u):
        idx, sem = ag_unit(u)

        @pl.when(u >= 2)
        def _():
            pltpu.make_async_copy(gathered.at[stage, idx], gathered.at[stage, idx], ag_recv.at[stage, sem]).wait()

        @pl.when(u == 2)
        def _():
            ag_copy(stage, 4).start()

        @pl.when(u == 3)
        def _():
            ag_copy(stage, 5).start()

        return idx

    def finish_sends(stage, with_stats):
        for n in range(6):
            rs_copy(stage, n).wait_send()
            ag_copy(stage, n).wait_send()
        if with_stats:
            for step in OTHERS:
                stat_copy(stage, step).wait_send()

    def normalized(stage, idx, gains, row):
        raw = gathered[stage, idx].astype(jnp.float32)
        scale = jnp.concatenate([scale_buf[...]] * (unit // HEAD_DIM), axis=1)
        return (raw * scale * gains[row:row + 1, span(idx)].astype(jnp.float32)).astype(jnp.bfloat16)

    def accumulate(which, hidden, weight):
        for col in range(0, ffn, 512):
            size = min(512, ffn - col)
            acc[which, col:col + size, :] += lax.dot_general(weight[col:col + size, :], hidden, (((1,), (1,)), ((), ())), preferred_element_type=jnp.float32)

    def out_part(n):
        wo_copy(n).wait()
        return jnp.dot(attn_ref[...], wo_buf[n], preferred_element_type=jnp.float32)

    def before_mlp():
        pl.loop(0, wd_slots)(lambda n: wd_copy(n).start())
        acc[...] = jnp.zeros_like(acc)
        res_copy.wait()

    gather_start(0, reduce_scatter(0, out_part, before_mlp))

    @pl.loop(0, 8)
    def _(u):
        idx = gather_wait(0, u)
        hidden = normalized(0, idx, gain_ref, layer)
        wait(gu_copies(u))
        slot = lax.rem(u, gu_slots)
        accumulate(0, hidden, wg_buf.at[slot])
        accumulate(1, hidden, wu_buf.at[slot])

        @pl.when(u + gu_slots < 8)
        def _():
            start(gu_copies(u + gu_slots))

    if not last:
        pl.loop(0, 2)(lambda u: start(qkv_copies(u)))
    for col in range(0, ffn, 256):
        size = min(256, ffn - col)
        gate = acc[0, col:col + 256, :]
        product = gate * lax.logistic(gate) * acc[1, col:col + 256, :]
        act[:, col:col + size] = jnp.transpose(product)[:, :size].astype(jnp.bfloat16)
    finish_sends(0, True)

    def down_part(n):
        wd_copy(n).wait()
        value = jnp.dot(act[...], wd_buf[lax.rem(n, wd_slots)], preferred_element_type=jnp.float32)

        @pl.when(n + wd_slots < 8)
        def _():
            wd_copy(n + wd_slots).start()

        return value

    if last:
        reduce_scatter(1, down_part, lambda: None)
        gather_start(1, None)

        def out_copy(idx):
            return pltpu.make_async_copy(gathered.at[1, idx], out_ref.at[:, span(idx)], out_sem.at[idx])

        pl.loop(0, 8)(lambda u: out_copy(gather_wait(1, u)).start())
        pl.loop(0, 8)(lambda idx: out_copy(idx).wait())
        finish_sends(1, False)
        return

    def before_qkv():
        qkv_acc[...] = jnp.zeros_like(qkv_acc)

    gather_start(1, reduce_scatter(1, down_part, before_qkv))
    cols = q_ref.shape[1]

    @pl.loop(0, 8)
    def _(u):
        idx = gather_wait(1, u)
        hidden = normalized(1, idx, gain2_ref, layer + 1)
        wait(qkv_copies(u))
        slot = lax.rem(u, 2)
        for which, buf in enumerate((wq_buf, wk_buf, wv_buf)):
            for col in range(0, cols, 512):
                part = slice(col, min(col + 512, cols))
                qkv_acc[which, :, part] += jnp.dot(hidden, buf[slot, :, part], preferred_element_type=jnp.float32)

        @pl.when(u + 2 < 8)
        def _():
            start(qkv_copies(u + 2))

    for head in range(0, cols, HEAD_DIM):
        lane = slice(head, head + HEAD_DIM)

        def biased(which, b_ref):
            return qkv_acc[which, :, lane] + b_ref[layer + 1:layer + 2, lane].astype(jnp.float32)

        def rope(proj):
            return (proj * cos_ref[...] + pltpu.roll(proj, HEAD_DIM // 2, 1) * sin_ref[...]).astype(jnp.bfloat16)

        q_ref[:, lane] = rope(biased(0, bq_ref))
        kv_ref[0, :, lane] = rope(biased(1, bk_ref))
        kv_ref[1, :, lane] = biased(2, bv_ref).astype(jnp.bfloat16)
    for half in (0, 1):
        res_out_ref[:, half * unit:(half + 1) * unit] = gathered[1, 2 * me + half]
    finish_sends(1, True)


def block(layer, last, collective_id, attn_out, residual, mlp_gain, attn_gain, cos_tab, sin_tab, w_out, w_gate, w_up, w_down,
          w_query, b_query, w_key, b_key, w_value, b_value):
    rows, cols = attn_out.shape
    width, ffn = w_gate.shape[1:]
    unit = width // 8
    bf, f32, dma, vmem = jnp.bfloat16, jnp.float32, pltpu.SemaphoreType.DMA, pltpu.VMEM
    any_spec, vmem_spec = pl.BlockSpec(memory_space=pl.ANY), pl.BlockSpec(memory_space=pltpu.VMEM)
    gu_slots, wd_slots = 2, 3
    args = [attn_out, residual, mlp_gain, w_out, jnp.swapaxes(w_gate, 1, 2), jnp.swapaxes(w_up, 1, 2), w_down]
    in_specs = [vmem_spec, any_spec, vmem_spec] + [any_spec] * 4
    scratch = [
        vmem((8, cols, unit), bf), vmem((gu_slots, ffn, unit), bf), vmem((gu_slots, ffn, unit), bf), vmem((wd_slots, ffn, unit), bf),
        vmem((2, -(-ffn // 256) * 256, rows), f32), vmem((rows, ffn), bf), vmem((6, rows, unit), bf), vmem((2, 6, rows, unit), bf),
        vmem((2, rows, unit), f32), vmem((2, 8, rows, unit), bf), vmem((rows, 2 * unit), bf), vmem((2, 4, 8, rows), f32), vmem((rows, HEAD_DIM), f32),
        dma(()), dma((8,)), dma((2, gu_slots)), dma((wd_slots,)), dma((2, 6)), dma((2, 6)), dma((2, 6)), dma((2, 6)), dma((2, 3)), dma((2, 4)),
    ]
    if last:
        out_shape, out_specs = jax.ShapeDtypeStruct((rows, width), bf), any_spec
        scratch.append(dma((8,)))
    else:
        args += [attn_gain, cos_tab, sin_tab]
        in_specs += [vmem_spec] * 3
        for w, b in ((w_query, b_query), (w_key, b_key), (w_value, b_value)):
            args += [w, b]
            in_specs += [any_spec, vmem_spec]
        out_shape = (jax.ShapeDtypeStruct((rows, 2 * unit), bf), jax.ShapeDtypeStruct((rows, cols), bf), jax.ShapeDtypeStruct((2, rows, cols), bf))
        out_specs = (vmem_spec,) * 3
        scratch += [vmem((2, unit, cols), bf)] * 3 + [vmem((3, rows, cols), f32), dma((3, 2))]
    return pl.pallas_call(
        functools.partial(block_kernel, layer, last),
        out_shape=out_shape,
        in_specs=in_specs,
        out_specs=out_specs,
        scratch_shapes=scratch,
        compiler_params=pltpu.CompilerParams(collective_id=collective_id, has_side_effects=True, vmem_limit_bytes=63 * MIB),
        cost_estimate=pl.CostEstimate(flops=2 * rows * width * (cols + 3 * ffn), bytes_accessed=2 * width * (cols + 3 * ffn), transcendentals=0),
        name='block',
    )(*args)


def solution(mesh):
    cp_size = mesh.shape['cp']

    def local_step(x_in, positions, attn_gain, mlp_gain, w_query, b_query, w_key, b_key, w_value, b_value, w_out, w_gate, w_up, w_down):
        block_dev = x_in.shape[0]
        cos_tab, sin_tab = rope_tables(positions)
        queries, kv_full = qkv_project(0, x_in, attn_gain, cos_tab, sin_tab, w_query, b_query, w_key, b_key, w_value, b_value)
        weights = (mlp_gain, attn_gain, cos_tab, sin_tab, w_out, w_gate, w_up, w_down, w_query, b_query, w_key, b_key, w_value, b_value)
        attn_out = attention(cp_size, block_dev * cp_size, 0, queries, kv_full)
        residual, queries, kv_win = block(0, False, 1, attn_out, x_in, *weights)
        attn_out = attention(cp_size, WINDOW, 2, queries, kv_win)
        hidden = block(1, True, 3, attn_out, residual, *weights)
        caches = [part.reshape(block_dev, -1, HEAD_DIM) for kv in (kv_full, kv_win) for part in (kv[0], kv[1])]
        return hidden, caches[0], caches[1], caches[2], caches[3]

    weight_col = P(None, None, 'tp')
    bias_col = P(None, 'tp')
    weight_row = P(None, 'tp', None)
    replicated = P(None, None)
    cache_spec = P('cp', 'tp', None)
    in_specs = (P('cp', None), P('cp'), replicated, replicated, weight_col, bias_col, weight_col, bias_col, weight_col, bias_col, weight_row, weight_col, weight_col, weight_row)
    out_specs = (P('cp', None), cache_spec, cache_spec, cache_spec, cache_spec)
    return jax.shard_map(local_step, mesh=mesh, in_specs=in_specs, out_specs=out_specs, check_vma=False)
```

```python
import functools

import jax
import jax.numpy as jnp
from jax import lax
from jax.experimental import pallas as pl
from jax.experimental.pallas import tpu as pltpu
from jax.sharding import PartitionSpec as P

HEAD_DIM = 128
WINDOW = 4096
MESH = pl.DeviceIdType.MESH
NEG = -0.7 * float(jnp.finfo(jnp.float32).max)
LOG2E = 1.4426950408889634
MIB = 1024 * 1024


def rms_norm(hidden, gain):
    hidden_f = hidden.astype(jnp.float32)
    variance = jnp.mean(hidden_f * hidden_f, axis=-1, keepdims=True)
    return (hidden_f * lax.rsqrt(variance + 1e-6) * gain.astype(jnp.float32)).astype(jnp.bfloat16)


def rope_tables(positions):
    inv_freq = 1.0 / (1000000.0 ** (jnp.arange(0, HEAD_DIM, 2, dtype=jnp.float32) / HEAD_DIM))
    angles = positions.astype(jnp.float32)[:, None] * inv_freq[None, :]
    cos, sin = jnp.cos(angles), jnp.sin(angles)
    return jnp.concatenate([cos, cos], axis=-1), jnp.concatenate([-sin, sin], axis=-1)


def qkv_kernel(layer, x_ref, gain_ref, cos_ref, sin_ref, wq_ref, bq_ref, wk_ref, bk_ref, wv_ref, bv_ref, q_ref, kv_ref, normed):
    @pl.when(pl.program_id(0) == 0)
    def _():
        normed[...] = rms_norm(x_ref[...], gain_ref[layer:layer + 1])

    hidden = normed[...]
    cos_tab, sin_tab = cos_ref[...], sin_ref[...]

    def project(w_ref, b_ref):
        return jnp.dot(hidden, w_ref[...], preferred_element_type=jnp.float32) + b_ref[layer:layer + 1].astype(jnp.float32)

    def rope(proj):
        heads = []
        for start in range(0, proj.shape[1], HEAD_DIM):
            head = proj[:, start:start + HEAD_DIM]
            heads.append(head * cos_tab + pltpu.roll(head, HEAD_DIM // 2, 1) * sin_tab)
        return jnp.concatenate(heads, axis=1).astype(jnp.bfloat16)

    q_ref[...] = rope(project(wq_ref, bq_ref))
    kv_ref[0] = rope(project(wk_ref, bk_ref))
    kv_ref[1] = project(wv_ref, bv_ref).astype(jnp.bfloat16)


def qkv_project(layer, hidden, gains, cos_tab, sin_tab, w_query, b_query, w_key, b_key, w_value, b_value, tile=256):
    rows, width = hidden.shape
    cols = w_query.shape[2]
    whole = lambda shape: pl.BlockSpec(shape, lambda n: (0,) * len(shape))
    weight = pl.BlockSpec((None, width, tile), lambda n: (layer, 0, n))
    bias = pl.BlockSpec((2, tile), lambda n: (0, n))
    return pl.pallas_call(
        functools.partial(qkv_kernel, layer),
        grid=(cols // tile,),
        out_shape=(jax.ShapeDtypeStruct((rows, cols), jnp.bfloat16), jax.ShapeDtypeStruct((2, rows, cols), jnp.bfloat16)),
        in_specs=[whole((rows, width)), whole((2, width)), whole(cos_tab.shape), whole(sin_tab.shape), weight, bias, weight, bias, weight, bias],
        out_specs=(pl.BlockSpec((rows, tile), lambda n: (0, n)), pl.BlockSpec((2, rows, tile), lambda n: (0, 0, n))),
        scratch_shapes=[pltpu.VMEM((rows, width), jnp.bfloat16)],
        compiler_params=pltpu.CompilerParams(vmem_limit_bytes=40 * MIB),
        cost_estimate=pl.CostEstimate(flops=6 * rows * width * cols, bytes_accessed=6 * width * cols, transcendentals=0),
        name='qkv',
    )(hidden, gains, cos_tab, sin_tab, w_query, b_query, w_key, b_key, w_value, b_value)


def attention_kernel(cp_size, window, q_ref, kv_ref, out_ref, kvbuf, qbuf, obuf, acc, m_buf, l_buf,
                     kv_send, kv_recv, fwd_send, q_send, q_recv, o_send, o_recv):
    rows = q_ref.shape[0]
    n_heads = q_ref.shape[1] // HEAD_DIM
    chips = cp_size // 2
    groups = cp_size // n_heads
    slots = cp_size // groups
    me = lax.axis_index('cp')
    chip, core = me // 2, lax.rem(me, 2)
    head, group = me // groups, lax.rem(me, groups)
    sibling = me + 1 - 2 * core
    scale = HEAD_DIM ** -0.5 * LOG2E

    def lanes(h):
        return pl.ds(pl.multiple_of(h * HEAD_DIM, HEAD_DIM), HEAD_DIM)

    def block_of(slot):
        odd = lax.rem(slot, 2)
        return 2 * groups * (slot // 2) + group + odd * (2 * groups - 1 - 2 * group)

    barrier = pltpu.get_barrier_semaphore()

    @pl.loop(1, cp_size)
    def _(step):
        pl.semaphore_signal(barrier, inc=1, device_id={'cp': lax.rem(me + step, cp_size)}, device_id_type=MESH)

    own_kv = pltpu.make_async_copy(kv_ref.at[:, :, lanes(head)], kvbuf.at[me], kv_recv.at[me])
    own_kv.start()
    pl.semaphore_wait(barrier, cp_size - 1)

    place = lax.rem(me, 2 * groups)
    upper = place // groups
    my_group = place + upper * (2 * groups - 1 - 2 * place)
    my_slot = 2 * (me // (2 * groups)) + upper

    def q_copy(h):
        return pltpu.make_async_remote_copy(q_ref.at[:, lanes(h)], qbuf.at[my_slot], q_send.at[h], q_recv.at[my_slot],
                                            device_id={'cp': groups * h + my_group}, device_id_type=MESH)

    def kv_copy(dst):
        return pltpu.make_async_remote_copy(kv_ref.at[:, :, lanes((2 * dst) // groups)], kvbuf.at[me], kv_send.at[dst], kv_recv.at[me],
                                            device_id={'cp': 2 * dst + core}, device_id_type=MESH)

    def fwd_copy(src):
        blk = 2 * src + core
        return pltpu.make_async_remote_copy(kvbuf.at[blk], kvbuf.at[blk], fwd_send.at[src], kv_recv.at[blk],
                                            device_id={'cp': sibling}, device_id_type=MESH)

    def kv_wait(blk):
        pltpu.make_async_copy(kvbuf.at[blk], kvbuf.at[blk], kv_recv.at[blk]).wait()

    @pl.loop(0, n_heads)
    def _(h):
        @pl.when(groups * h + my_group != me)
        def _():
            q_copy(h).start()

        @pl.when(groups * h + my_group == me)
        def _():
            pltpu.make_async_copy(q_ref.at[:, lanes(h)], qbuf.at[my_slot], q_recv.at[my_slot]).start()

    @pl.loop(1, chips)
    def _(step):
        kv_copy(lax.rem(chip + step, chips)).start()

    kv_wait(me)
    fwd_copy(chip).start()

    acc[...] = jnp.zeros_like(acc)
    l_buf[...] = jnp.zeros_like(l_buf)
    m_buf[...] = jnp.full_like(m_buf, NEG)

    @pl.loop(0, slots)
    def _(slot):
        pltpu.make_async_copy(qbuf.at[slot], qbuf.at[slot], q_recv.at[slot]).wait()

    def attend(slot, src, masked):
        keys = kvbuf[pl.ds(2 * src, 2), 0].reshape(2 * rows, HEAD_DIM)
        values = kvbuf[pl.ds(2 * src, 2), 1].reshape(2 * rows, HEAD_DIM)
        scores = lax.dot_general(qbuf[slot], keys, (((1,), (1,)), ((), ())), preferred_element_type=jnp.float32) * scale
        if masked:
            q_pos = block_of(slot) * rows + lax.broadcasted_iota(jnp.int32, scores.shape, 0)
            k_pos = src * 2 * rows + lax.broadcasted_iota(jnp.int32, scores.shape, 1)
            scores = jnp.where((k_pos <= q_pos) & (k_pos > q_pos - window), scores, NEG)
        parts = [scores[:, i:i + HEAD_DIM] for i in range(0, scores.shape[1], HEAD_DIM)] if scores.shape[1] % HEAD_DIM == 0 else [scores]
        m_prev = m_buf[slot]
        m_lane = functools.reduce(jnp.maximum, parts)
        m_new = jnp.maximum(m_prev, jnp.max(m_lane, axis=1, keepdims=True))
        alpha = jnp.exp2(m_prev - m_new)
        probs = [jnp.exp2(part - m_new[:, :part.shape[1]]) for part in parts]
        l_new = functools.reduce(jnp.add, probs)
        if l_new.shape[1] != HEAD_DIM:
            l_new = jnp.concatenate([l_new, jnp.zeros((rows, HEAD_DIM - l_new.shape[1]), jnp.float32)], axis=1)
        l_buf[slot] = alpha * l_buf[slot] + l_new
        m_buf[slot] = m_new
        probs_bf = jnp.concatenate([part.astype(jnp.bfloat16) for part in probs], axis=1)
        acc[slot] = alpha * acc[slot] + jnp.dot(probs_bf, values, preferred_element_type=jnp.float32)

    win_blocks = window // rows

    @pl.loop(1, chips + 1)
    def _(step):
        @pl.when(step < chips)
        def _():
            src = lax.rem(chip - step + chips, chips)
            kv_wait(2 * src + core)
            fwd_copy(src).start()

        src = lax.rem(chip - step + 1 + chips, chips)
        kv_wait(2 * src + 1 - core)

        @pl.loop(0, slots)
        def _(slot):
            blk = block_of(slot)
            diagonal = src == blk // 2
            edge = 2 * src <= blk - win_blocks
            inside = (2 * src <= blk) & (2 * src + 1 >= blk - win_blocks)

            @pl.when(inside & jnp.logical_not(diagonal | edge))
            def _():
                attend(slot, src, False)

            @pl.when(inside & (diagonal | edge))
            def _():
                attend(slot, src, True)

    def o_copy(slot):
        return pltpu.make_async_remote_copy(obuf.at[slot], out_ref.at[:, lanes(head)], o_send.at[slot], o_recv.at[head],
                                            device_id={'cp': block_of(slot)}, device_id_type=MESH)

    @pl.loop(0, slots)
    def _(slot):
        total = jnp.sum(l_buf[slot], axis=1, keepdims=True)
        obuf[slot] = (acc[slot] / total).astype(jnp.bfloat16)

        @pl.when(block_of(slot) != me)
        def _():
            o_copy(slot).start()

        @pl.when(block_of(slot) == me)
        def _():
            pltpu.make_async_copy(obuf.at[slot], out_ref.at[:, lanes(head)], o_recv.at[head]).start()

    @pl.loop(0, n_heads)
    def _(h):
        pltpu.make_async_copy(out_ref.at[:, lanes(h)], out_ref.at[:, lanes(h)], o_recv.at[h]).wait()

        @pl.when(groups * h + my_group != me)
        def _():
            q_copy(h).wait_send()

    @pl.loop(0, slots)
    def _(slot):
        @pl.when(block_of(slot) != me)
        def _():
            o_copy(slot).wait_send()

    @pl.loop(0, chips)
    def _(dst):
        fwd_copy(dst).wait_send()

        @pl.when(dst != chip)
        def _():
            kv_copy(dst).wait_send()


def attention(cp_size, window, collective_id, queries, kv):
    rows, cols = queries.shape
    n_heads = cols // HEAD_DIM
    slots = n_heads
    dma = pltpu.SemaphoreType.DMA
    any_spec = pl.BlockSpec(memory_space=pl.ANY)
    return pl.pallas_call(
        functools.partial(attention_kernel, cp_size, window),
        out_shape=jax.ShapeDtypeStruct((rows, cols), jnp.bfloat16),
        in_specs=[any_spec, any_spec],
        out_specs=any_spec,
        scratch_shapes=[
            pltpu.VMEM((cp_size, 2, rows, HEAD_DIM), jnp.bfloat16),
            pltpu.VMEM((slots, rows, HEAD_DIM), jnp.bfloat16),
            pltpu.VMEM((slots, rows, HEAD_DIM), jnp.bfloat16),
            pltpu.VMEM((slots, rows, HEAD_DIM), jnp.float32),
            pltpu.VMEM((slots, rows, HEAD_DIM), jnp.float32),
            pltpu.VMEM((slots, rows, HEAD_DIM), jnp.float32),
            dma((cp_size // 2,)), dma((cp_size,)), dma((cp_size // 2,)),
            dma((n_heads,)), dma((slots,)), dma((slots,)), dma((n_heads,)),
        ],
        compiler_params=pltpu.CompilerParams(collective_id=collective_id, has_side_effects=True, vmem_limit_bytes=24 * MIB),
        cost_estimate=pl.CostEstimate(flops=4 * 132 * rows * rows * HEAD_DIM, bytes_accessed=8 * MIB, transcendentals=132 * rows * rows),
        name='attention',
    )(queries, kv)


def block_kernel(layer, last, *refs):
    if last:
        (attn_ref, res_ref, gain_ref, wo_ref, wg_ref, wu_ref, wd_ref, out_ref,
         wo_buf, wg_buf, wu_buf, wd_buf, acc, act, sbuf, rbuf, own, gathered, res_buf, stats, scale_buf,
         res_sem, wo_sem, gu_sem, wd_sem, rs_send, rs_recv, ag_send, ag_recv, st_send, st_recv, out_sem) = refs
    else:
        (attn_ref, res_ref, gain_ref, wo_ref, wg_ref, wu_ref, wd_ref,
         gain2_ref, cos_ref, sin_ref, wq_ref, bq_ref, wk_ref, bk_ref, wv_ref, bv_ref,
         res_out_ref, q_ref, kv_ref,
         wo_buf, wg_buf, wu_buf, wd_buf, acc, act, sbuf, rbuf, own, gathered, res_buf, stats, scale_buf,
         res_sem, wo_sem, gu_sem, wd_sem, rs_send, rs_recv, ag_send, ag_recv, st_send, st_recv,
         wq_buf, wk_buf, wv_buf, qkv_acc, qkv_sem) = refs
    rows, unit = own.shape[1], own.shape[2]
    width = 8 * unit
    ffn = act.shape[1]
    me = lax.axis_index('tp')
    gu_slots, wd_slots = wg_buf.shape[0], wd_buf.shape[0]

    def rs_unit(n):
        pair, odd = n // 2, lax.rem(n, 2)
        mid, first = (pair * (3 - pair)) // 2, (3 - pair) // 3
        half = odd + mid * (2 - pair) * (1 - 2 * odd)
        return 2 * lax.rem(me + 2 * first + mid * (1 + 2 * odd), 4) + half

    def ag_unit(u):
        pair, odd = u // 2, lax.rem(u, 2)
        mid, final = (pair * (3 - pair)) // 2, pair // 3
        half = odd + mid * (pair - 1) * (1 - 2 * odd)
        return 2 * lax.rem(me + mid * (3 - 2 * odd) + 2 * final, 4) + half, mid * (pair - 1 + 2 * odd) + final * (4 + odd)

    def span(idx):
        return pl.ds(pl.multiple_of(idx * unit, unit), unit)

    def wo_copy(n):
        return pltpu.make_async_copy(wo_ref.at[layer, :, span(rs_unit(n))], wo_buf.at[n], wo_sem.at[n])

    def gu_copies(u):
        idx, slot = ag_unit(u)[0], lax.rem(u, gu_slots)
        return (pltpu.make_async_copy(wg_ref.at[layer, :, span(idx)], wg_buf.at[slot], gu_sem.at[0, slot]),
                pltpu.make_async_copy(wu_ref.at[layer, :, span(idx)], wu_buf.at[slot], gu_sem.at[1, slot]))

    def wd_copy(n):
        slot = lax.rem(n, wd_slots)
        return pltpu.make_async_copy(wd_ref.at[layer, :, span(rs_unit(n))], wd_buf.at[slot], wd_sem.at[slot])

    def qkv_copies(u):
        idx, slot = ag_unit(u)[0], lax.rem(u, 2)
        return tuple(pltpu.make_async_copy(w.at[layer + 1, span(idx), :], buf.at[slot], qkv_sem.at[i, slot])
                     for i, (w, buf) in enumerate(((wq_ref, wq_buf), (wk_ref, wk_buf), (wv_ref, wv_buf))))

    def start(copies):
        for copy in copies:
            copy.start()

    def wait(copies):
        for copy in copies:
            copy.wait()

    barrier = pltpu.get_barrier_semaphore()
    for step in (1, 2, 3):
        pl.semaphore_signal(barrier, inc=1, device_id={'tp': lax.rem(me + step, 4)}, device_id_type=MESH)
    first_col = 2 * me * unit if res_ref.shape[1] == width else 0
    res_copy = pltpu.make_async_copy(res_ref.at[:, pl.ds(pl.multiple_of(first_col, unit), 2 * unit)], res_buf, res_sem)
    pl.loop(0, 8)(lambda n: wo_copy(n).start())
    res_copy.start()
    pl.loop(0, gu_slots)(lambda u: start(gu_copies(u)))
    pl.semaphore_wait(barrier, 3)

    def rs_copy(stage, n):
        return pltpu.make_async_remote_copy(sbuf.at[n], rbuf.at[stage, n], rs_send.at[stage, n], rs_recv.at[stage, n],
                                            device_id={'tp': lax.rem(me + 1 + 2 * lax.rem(n, 2), 4)}, device_id_type=MESH)

    def reduce_scatter(stage, part, after):
        @pl.loop(0, 8)
        def _(n):
            value = part(n)

            @pl.when(n < 4)
            def _():
                sbuf[n] = value.astype(jnp.bfloat16)
                rs_copy(stage, n).start()

            @pl.when((n >= 4) & (n < 6))
            def _():
                rs_copy(stage, n - 4).wait_recv()
                sbuf[n] = (value + rbuf[stage, n - 4].astype(jnp.float32)).astype(jnp.bfloat16)
                rs_copy(stage, n).start()

            @pl.when(n >= 6)
            def _():
                own[n - 6] = value

        after()
        square = jnp.zeros((rows, HEAD_DIM), jnp.float32)
        for half in (0, 1):
            from_left, from_right = (4, 3) if half == 0 else (2, 5)
            rs_copy(stage, from_left).wait_recv()
            rs_copy(stage, from_right).wait_recv()
            residual = res_buf[:, half * unit:(half + 1) * unit] if stage == 0 else gathered[0, 2 * me + half]
            total = own[half] + rbuf[stage, from_left].astype(jnp.float32) + rbuf[stage, from_right].astype(jnp.float32)
            new = (residual.astype(jnp.float32) + total).astype(jnp.bfloat16)
            gathered[stage, 2 * me + half] = new
            new_f = new.astype(jnp.float32)
            for lane in range(0, unit, HEAD_DIM):
                square = square + new_f[:, lane:lane + HEAD_DIM] * new_f[:, lane:lane + HEAD_DIM]
        return square

    def stat_copy(stage, step):
        return pltpu.make_async_remote_copy(stats.at[stage, me], stats.at[stage, me], st_send.at[stage, step - 1], st_recv.at[stage, me],
                                            device_id={'tp': lax.rem(me + step, 4)}, device_id_type=MESH)

    def ag_copy(stage, s):
        if s < 4:
            idx = 2 * me + (0, 1, 1, 0)[s]
        else:
            idx = 2 * lax.rem(me + 3, 4) if s == 4 else 2 * lax.rem(me + 1, 4) + 1
        to = lax.rem(me + (1, 1, 3, 3, 1, 3)[s], 4)
        return pltpu.make_async_remote_copy(gathered.at[stage, idx], gathered.at[stage, idx], ag_send.at[stage, s], ag_recv.at[stage, s],
                                            device_id={'tp': to}, device_id_type=MESH)

    def gather_start(stage, square):
        if square is not None:
            total = jnp.broadcast_to(jnp.sum(square, axis=1, keepdims=True), square.shape)
            stats[stage, me] = jnp.transpose(total)[:8]
            for step in (1, 2, 3):
                stat_copy(stage, step).start()
        for s in (0, 2, 1, 3):
            ag_copy(stage, s).start()
        if square is not None:
            for step in (1, 2, 3):
                source = lax.rem(me + step, 4)
                pltpu.make_async_copy(stats.at[stage, source], stats.at[stage, source], st_recv.at[stage, source]).wait()
            total = stats[stage, 0] + stats[stage, 1] + stats[stage, 2] + stats[stage, 3]
            inverse = lax.rsqrt(total[:1] / width + 1e-6)
            scale_buf[...] = jnp.transpose(jnp.broadcast_to(inverse, (HEAD_DIM, rows)))

    def gather_wait(stage, u):
        idx, sem = ag_unit(u)

        @pl.when(u >= 2)
        def _():
            pltpu.make_async_copy(gathered.at[stage, idx], gathered.at[stage, idx], ag_recv.at[stage, sem]).wait()

        @pl.when(u == 2)
        def _():
            ag_copy(stage, 4).start()

        @pl.when(u == 3)
        def _():
            ag_copy(stage, 5).start()

        return idx

    def finish_sends(stage, with_stats):
        for n in range(6):
            rs_copy(stage, n).wait_send()
            ag_copy(stage, n).wait_send()
        if with_stats:
            for step in (1, 2, 3):
                stat_copy(stage, step).wait_send()

    def normalized(stage, idx, gains, row):
        raw = gathered[stage, idx].astype(jnp.float32)
        scale = jnp.concatenate([scale_buf[...]] * (unit // HEAD_DIM), axis=1)
        return (raw * scale * gains[row:row + 1, span(idx)].astype(jnp.float32)).astype(jnp.bfloat16)

    def accumulate(which, hidden, weight):
        for col in range(0, ffn, 512):
            size = min(512, ffn - col)
            acc[which, col:col + size, :] += lax.dot_general(weight[col:col + size, :], hidden, (((1,), (1,)), ((), ())), preferred_element_type=jnp.float32)

    def out_part(n):
        wo_copy(n).wait()
        return jnp.dot(attn_ref[...], wo_buf[n], preferred_element_type=jnp.float32)

    def before_mlp():
        pl.loop(0, wd_slots)(lambda n: wd_copy(n).start())
        acc[...] = jnp.zeros_like(acc)
        res_copy.wait()

    gather_start(0, reduce_scatter(0, out_part, before_mlp))

    @pl.loop(0, 8)
    def _(u):
        idx = gather_wait(0, u)
        hidden = normalized(0, idx, gain_ref, layer)
        wait(gu_copies(u))
        slot = lax.rem(u, gu_slots)
        accumulate(0, hidden, wg_buf.at[slot])
        accumulate(1, hidden, wu_buf.at[slot])

        @pl.when(u + gu_slots < 8)
        def _():
            start(gu_copies(u + gu_slots))

    if not last:
        pl.loop(0, 2)(lambda u: start(qkv_copies(u)))
    for col in range(0, ffn, 256):
        size = min(256, ffn - col)
        gate = acc[0, col:col + 256, :]
        product = gate * lax.logistic(gate) * acc[1, col:col + 256, :]
        act[:, col:col + size] = jnp.transpose(product)[:, :size].astype(jnp.bfloat16)
    finish_sends(0, True)

    def down_part(n):
        wd_copy(n).wait()
        value = jnp.dot(act[...], wd_buf[lax.rem(n, wd_slots)], preferred_element_type=jnp.float32)

        @pl.when(n + wd_slots < 8)
        def _():
            wd_copy(n + wd_slots).start()

        return value

    if last:
        reduce_scatter(1, down_part, lambda: None)
        gather_start(1, None)

        def out_copy(idx):
            return pltpu.make_async_copy(gathered.at[1, idx], out_ref.at[:, span(idx)], out_sem.at[idx])

        pl.loop(0, 8)(lambda u: out_copy(gather_wait(1, u)).start())
        pl.loop(0, 8)(lambda idx: out_copy(idx).wait())
        finish_sends(1, False)
        return

    def before_qkv():
        qkv_acc[...] = jnp.zeros_like(qkv_acc)

    gather_start(1, reduce_scatter(1, down_part, before_qkv))
    cols = q_ref.shape[1]

    @pl.loop(0, 8)
    def _(u):
        idx = gather_wait(1, u)
        hidden = normalized(1, idx, gain2_ref, layer + 1)
        wait(qkv_copies(u))
        slot = lax.rem(u, 2)
        for which, buf in enumerate((wq_buf, wk_buf, wv_buf)):
            for col in range(0, cols, 512):
                part = slice(col, min(col + 512, cols))
                qkv_acc[which, :, part] += jnp.dot(hidden, buf[slot, :, part], preferred_element_type=jnp.float32)

        @pl.when(u + 2 < 8)
        def _():
            start(qkv_copies(u + 2))

    for head in range(0, cols, HEAD_DIM):
        lane = slice(head, head + HEAD_DIM)

        def biased(which, b_ref):
            return qkv_acc[which, :, lane] + b_ref[layer + 1:layer + 2, lane].astype(jnp.float32)

        def rope(proj):
            return (proj * cos_ref[...] + pltpu.roll(proj, HEAD_DIM // 2, 1) * sin_ref[...]).astype(jnp.bfloat16)

        q_ref[:, lane] = rope(biased(0, bq_ref))
        kv_ref[0, :, lane] = rope(biased(1, bk_ref))
        kv_ref[1, :, lane] = biased(2, bv_ref).astype(jnp.bfloat16)
    for half in (0, 1):
        res_out_ref[:, half * unit:(half + 1) * unit] = gathered[1, 2 * me + half]
    finish_sends(1, True)


def block(layer, last, collective_id, attn_out, residual, mlp_gain, attn_gain, cos_tab, sin_tab, w_out, w_gate, w_up, w_down,
          w_query, b_query, w_key, b_key, w_value, b_value):
    rows, cols = attn_out.shape
    width, ffn = w_gate.shape[1:]
    unit = width // 8
    bf, f32, dma, vmem = jnp.bfloat16, jnp.float32, pltpu.SemaphoreType.DMA, pltpu.VMEM
    any_spec, vmem_spec = pl.BlockSpec(memory_space=pl.ANY), pl.BlockSpec(memory_space=pltpu.VMEM)
    gu_slots, wd_slots = 2, 3
    args = [attn_out, residual, mlp_gain, w_out, jnp.swapaxes(w_gate, 1, 2), jnp.swapaxes(w_up, 1, 2), w_down]
    in_specs = [vmem_spec, any_spec, vmem_spec] + [any_spec] * 4
    scratch = [
        vmem((8, cols, unit), bf), vmem((gu_slots, ffn, unit), bf), vmem((gu_slots, ffn, unit), bf), vmem((wd_slots, ffn, unit), bf),
        vmem((2, -(-ffn // 256) * 256, rows), f32), vmem((rows, ffn), bf), vmem((6, rows, unit), bf), vmem((2, 6, rows, unit), bf),
        vmem((2, rows, unit), f32), vmem((2, 8, rows, unit), bf), vmem((rows, 2 * unit), bf), vmem((2, 4, 8, rows), f32), vmem((rows, HEAD_DIM), f32),
        dma(()), dma((8,)), dma((2, gu_slots)), dma((wd_slots,)), dma((2, 6)), dma((2, 6)), dma((2, 6)), dma((2, 6)), dma((2, 3)), dma((2, 4)),
    ]
    if last:
        out_shape, out_specs = jax.ShapeDtypeStruct((rows, width), bf), any_spec
        scratch.append(dma((8,)))
    else:
        args += [attn_gain, cos_tab, sin_tab]
        in_specs += [vmem_spec] * 3
        for w, b in ((w_query, b_query), (w_key, b_key), (w_value, b_value)):
            args += [w, b]
            in_specs += [any_spec, vmem_spec]
        out_shape = (jax.ShapeDtypeStruct((rows, 2 * unit), bf), jax.ShapeDtypeStruct((rows, cols), bf), jax.ShapeDtypeStruct((2, rows, cols), bf))
        out_specs = (vmem_spec,) * 3
        scratch += [vmem((2, unit, cols), bf)] * 3 + [vmem((3, rows, cols), f32), dma((3, 2))]
    return pl.pallas_call(
        functools.partial(block_kernel, layer, last),
        out_shape=out_shape,
        in_specs=in_specs,
        out_specs=out_specs,
        scratch_shapes=scratch,
        compiler_params=pltpu.CompilerParams(collective_id=collective_id, has_side_effects=True, vmem_limit_bytes=63 * MIB),
        cost_estimate=pl.CostEstimate(flops=2 * rows * width * (cols + 3 * ffn), bytes_accessed=2 * width * (cols + 3 * ffn), transcendentals=0),
        name='block',
    )(*args)


def solution(mesh):
    cp_size = mesh.shape['cp']

    def local_step(x_in, positions, attn_gain, mlp_gain, w_query, b_query, w_key, b_key, w_value, b_value, w_out, w_gate, w_up, w_down):
        block_dev = x_in.shape[0]
        cos_tab, sin_tab = rope_tables(positions)
        queries, kv_full = qkv_project(0, x_in, attn_gain, cos_tab, sin_tab, w_query, b_query, w_key, b_key, w_value, b_value)
        weights = (mlp_gain, attn_gain, cos_tab, sin_tab, w_out, w_gate, w_up, w_down, w_query, b_query, w_key, b_key, w_value, b_value)
        attn_out = attention(cp_size, block_dev * cp_size, 0, queries, kv_full)
        residual, queries, kv_win = block(0, False, 1, attn_out, x_in, *weights)
        attn_out = attention(cp_size, WINDOW, 2, queries, kv_win)
        hidden = block(1, True, 3, attn_out, residual, *weights)
        caches = [part.reshape(block_dev, -1, HEAD_DIM) for kv in (kv_full, kv_win) for part in (kv[0], kv[1])]
        return hidden, caches[0], caches[1], caches[2], caches[3]

    weight_col = P(None, None, 'tp')
    bias_col = P(None, 'tp')
    weight_row = P(None, 'tp', None)
    replicated = P(None, None)
    cache_spec = P('cp', 'tp', None)
    in_specs = (P('cp', None), P('cp'), replicated, replicated, weight_col, bias_col, weight_col, bias_col, weight_col, bias_col, weight_row, weight_col, weight_col, weight_row)
    out_specs = (P('cp', None), cache_spec, cache_spec, cache_spec, cache_spec)
    return jax.shard_map(local_step, mesh=mesh, in_specs=in_specs, out_specs=out_specs, check_vma=False)
```
